128 devices in a mesh: tp: 2 (over core), fsdp: 64 (over z, y, x).
Axes of the slice: x: 4, y: 4, z: 4, core: 2. Of those that a mesh axis runs over, the one named last changes fastest.
Arguments:
- emb_table: float32 [16384, 1152], P('tp', 'fsdp')
- tok_ids: int32 [64, 1024], P('fsdp')
- lab_ids: int32 [64, 1024], P('fsdp')
- h_last: bfloat16 [64, 1024, 1152], P('fsdp')
- g_embed: bfloat16 [64, 1024, 1152], P('fsdp')
- norm_w: float32 [1152], P('fsdp')
Outputs:
- output 1: bfloat16 [64, 1024, 1152], P('fsdp')
- output 2: float32 [], replicated
- output 3: bfloat16 [64, 1024, 1152], P('fsdp')
- output 4: float32 [1152], P('fsdp')
- output 5: float32 [16384, 1152], P('tp', 'fsdp')
All inputs are finite; a program needn't handle non-finite values.
Results may differ from the reference program's by a relative error of at most 0.001.
Values are sent between devices in bfloat16 or wider.
A program may use at most 1 GiB of HBM per device.

```python
import math
import jax
import jax.numpy as jnp
from jax import lax

D = 1152
VOCAB = 16384
BATCH = 64
SEQ = 1024

SOFT_CAP = 30.0
NORM_EPS = 1e-6
TOKENS = BATCH * SEQ
LEVELS = VOCAB.bit_length()
GRAD_STD = 12.0 / (TOKENS * math.sqrt(D))


def setup_inputs(seed: int = 0) -> dict:
    key_list = jax.random.split(jax.random.key(seed), 7)
    emb_table = jax.random.normal(key_list[0], (VOCAB, D), jnp.float32) * D ** -0.5
    tok_level = jax.random.randint(key_list[1], (BATCH, SEQ), 0, LEVELS)
    tok_upper = jnp.minimum(jnp.left_shift(jnp.full((BATCH, SEQ), 2, jnp.int32), tok_level), VOCAB)
    tok_ids = jax.random.randint(key_list[2], (BATCH, SEQ), 0, tok_upper)
    tok_ids = tok_ids.at[0, 0].set(VOCAB - 1).at[0, 1].set(0)
    lab_ids = jax.random.randint(key_list[3], (BATCH, SEQ), 0, VOCAB)
    lab_ids = lab_ids.at[BATCH - 1, SEQ - 1].set(VOCAB - 1).at[BATCH - 1, SEQ - 2].set(0)
    h_last = jax.random.normal(key_list[4], (BATCH, SEQ, D), jnp.float32).astype(jnp.bfloat16)
    g_embed = (jax.random.normal(key_list[5], (BATCH, SEQ, D), jnp.float32) * GRAD_STD).astype(jnp.bfloat16)
    norm_w = 15.0 + 5.0 * jax.random.normal(key_list[6], (D,), jnp.float32)
    return {"emb_table": emb_table, "tok_ids": tok_ids, "lab_ids": lab_ids, "h_last": h_last, "g_embed": g_embed, "norm_w": norm_w}


def reference(emb_table, tok_ids, lab_ids, h_last, g_embed, norm_w):
    table_bf = emb_table.astype(jnp.bfloat16)
    emb_scale = jnp.asarray(math.sqrt(D), jnp.bfloat16).astype(jnp.float32)
    x_emb = (jnp.take(table_bf, tok_ids, axis=0).astype(jnp.float32) * emb_scale).astype(jnp.bfloat16)
    norm_gain = 1.0 + norm_w
    vocab_ids = jnp.arange(VOCAB, dtype=jnp.int32)

    def row_step(d_acc, row_in):
        h_row, lab_row = row_in
        h_wide = h_row.astype(jnp.float32)
        inv_rms = lax.rsqrt(jnp.mean(h_wide * h_wide, axis=1, keepdims=True) + NORM_EPS)
        h_norm = h_wide * inv_rms
        x_norm = (h_norm * norm_gain).astype(jnp.bfloat16)
        logits = jnp.dot(x_norm, table_bf.T, preferred_element_type=jnp.float32)
        tanh_z = jnp.tanh(logits / SOFT_CAP)
        capped = SOFT_CAP * tanh_z
        log_norm = jax.nn.logsumexp(capped, axis=1)
        lab_hit = lab_row[:, None] == vocab_ids[None, :]
        lab_logit = jnp.sum(jnp.where(lab_hit, capped, 0.0), axis=1)
        soft_prob = jnp.exp(capped - log_norm[:, None])
        d_logits = ((soft_prob - lab_hit.astype(jnp.float32)) * (1.0 - tanh_z * tanh_z) / TOKENS).astype(jnp.bfloat16)
        d_xnorm = jnp.dot(d_logits, table_bf, preferred_element_type=jnp.float32)
        g_dir = d_xnorm * norm_gain
        d_hid = (inv_rms * (g_dir - h_norm * jnp.mean(g_dir * h_norm, axis=1, keepdims=True))).astype(jnp.bfloat16)
        d_gain = jnp.sum(d_xnorm * h_norm, axis=0)
        d_acc = d_acc + jnp.dot(d_logits.T, x_norm, preferred_element_type=jnp.float32)
        return d_acc, (jnp.sum(log_norm - lab_logit), d_hid, d_gain)

    d_head, (loss_rows, d_hidden, gain_rows) = lax.scan(row_step, jnp.zeros((VOCAB, D), jnp.float32), (h_last, lab_ids))
    loss_val = jnp.sum(loss_rows) / TOKENS
    d_norm_w = jnp.sum(gain_rows, axis=0)
    scaled_grad = (g_embed.astype(jnp.float32) * emb_scale).reshape(TOKENS, D)
    d_look = jax.ops.segment_sum(scaled_grad, tok_ids.reshape(TOKENS), num_segments=VOCAB)
    d_table = d_head + d_look
    return (x_emb, loss_val, d_hidden, d_norm_w, d_table)
```

```python
import math
import jax
import jax.numpy as jnp
from jax import lax
from jax.sharding import PartitionSpec as P

SOFT_CAP = 30.0
NORM_EPS = 1e-6
XN = 4


def solution(mesh):
    fsdp_size = mesh.shape["fsdp"]
    groups = fsdp_size // XN
    x_groups = [[i * XN + j for j in range(XN)] for i in range(groups)]

    def device_step(emb_shard, tok_ids, lab_ids, h_last, g_embed, norm_w):
        vocab_rows, cols = emb_shard.shape
        batch_loc, seq_len, width = h_last.shape
        tok_count = batch_loc * seq_len
        total_tokens = tok_count * fsdp_size
        quarter = vocab_rows // XN
        row_start = lax.axis_index("tp") * vocab_rows
        me = lax.axis_index("fsdp")
        vocab_iota = jnp.arange(vocab_rows, dtype=jnp.int32)
        emb_scale = jnp.asarray(math.sqrt(width), jnp.bfloat16).astype(jnp.float32)

        piece = emb_shard.T.astype(jnp.bfloat16).reshape(cols, XN, quarter).transpose(1, 0, 2)
        piece = lax.all_to_all(piece, "fsdp", split_axis=0, concat_axis=0, axis_index_groups=x_groups)
        piece = piece.reshape(XN * cols, quarter)
        table = lax.all_gather(piece, "fsdp", axis=0)
        table = table.reshape(groups, XN, XN * cols, quarter).transpose(0, 2, 1, 3).reshape(width, vocab_rows)

        tok_local = tok_ids.reshape(tok_count) - row_start
        tok_hit = (tok_local[:, None] == vocab_iota[None, :]).astype(jnp.bfloat16)
        row_vals = jnp.einsum("tv,dv->td", tok_hit, table, preferred_element_type=jnp.float32).astype(jnp.bfloat16)
        row_vals = lax.psum(row_vals, "tp")
        x_emb = (row_vals.astype(jnp.float32) * emb_scale).astype(jnp.bfloat16)

        mine = jnp.where(lax.axis_index("tp") == 0, norm_w, 0.0)
        norm_full = lax.dynamic_update_slice(jnp.zeros((width,), jnp.float32), mine, (me * cols,))
        norm_gain = 1.0 + lax.psum(norm_full, ("tp", "fsdp"))
        h_wide = h_last.reshape(tok_count, width).astype(jnp.float32)
        inv_rms = lax.rsqrt(jnp.mean(h_wide * h_wide, axis=1, keepdims=True) + NORM_EPS)
        h_norm = h_wide * inv_rms
        x_norm = (h_norm * norm_gain).astype(jnp.bfloat16)

        logits = jnp.einsum("td,dv->tv", x_norm, table, preferred_element_type=jnp.float32)
        tanh_z = jnp.tanh(logits / SOFT_CAP)
        capped = SOFT_CAP * tanh_z
        exp_shift = jnp.exp(capped - SOFT_CAP)
        lab_hit = (lab_ids.reshape(tok_count) - row_start)[:, None] == vocab_iota[None, :]
        tok_stats = jnp.stack([jnp.sum(exp_shift, axis=1), jnp.sum(jnp.where(lab_hit, capped, 0.0), axis=1)])
        tok_stats = lax.psum(tok_stats, "tp")
        sum_exp = tok_stats[0]
        log_norm = jnp.log(sum_exp) + SOFT_CAP
        loss_part = 0.5 * jnp.sum(log_norm - tok_stats[1])

        soft_prob = exp_shift / sum_exp[:, None]
        d_logits = ((soft_prob - lab_hit.astype(jnp.float32)) * (1.0 - tanh_z * tanh_z) / total_tokens).astype(jnp.bfloat16)
        d_part = jnp.einsum("tv,dv->td", d_logits, table, preferred_element_type=jnp.float32)
        d_xnorm = lax.psum(d_part, "tp")
        g_dir = d_xnorm * norm_gain
        d_hidden = (inv_rms * (g_dir - h_norm * jnp.mean(g_dir * h_norm, axis=1, keepdims=True))).astype(jnp.bfloat16)
        small = jnp.concatenate([jnp.sum(d_part * h_norm, axis=0), loss_part[None]])
        small = lax.psum(small, ("tp", "fsdp"))
        loss_val = small[width] / total_tokens
        d_norm_w = lax.dynamic_slice(small, (me * cols,), (cols,))

        both_l = jnp.concatenate([d_logits, (tok_hit * emb_scale.astype(jnp.bfloat16))], axis=0)
        both_x = jnp.concatenate([x_norm, g_embed.reshape(tok_count, width)], axis=0)
        grad = jnp.einsum("tv,td->dv", both_l, both_x, preferred_element_type=jnp.float32)
        grad = grad.reshape(groups, XN * cols, XN, quarter).transpose(0, 2, 1, 3).reshape(fsdp_size, XN * cols, quarter)
        grad = lax.psum_scatter(grad, "fsdp", scatter_dimension=0)
        grad = lax.all_to_all(grad.reshape(XN, cols, quarter), "fsdp", split_axis=0, concat_axis=0, axis_index_groups=x_groups)
        d_table = grad.transpose(1, 0, 2).reshape(cols, vocab_rows).T
        return (x_emb.reshape(batch_loc, seq_len, width), loss_val, d_hidden.reshape(batch_loc, seq_len, width), d_norm_w, d_table)

    spec_tok = P("fsdp", None)
    spec_act = P("fsdp", None, None)
    return jax.shard_map(device_step, mesh=mesh, in_specs=(P("tp", "fsdp"), spec_tok, spec_tok, spec_act, spec_act, P("fsdp")), out_specs=(spec_act, P(), spec_act, P("fsdp"), P("tp", "fsdp")), check_vma=False)
```

```python
import functools
import math
import jax
import jax.numpy as jnp
from jax import lax
from jax.experimental import pallas as pl
from jax.experimental.pallas import tpu as pltpu
from jax.sharding import PartitionSpec as P

SOFT_CAP = 30.0
NORM_EPS = 1e-6
MESH = pl.DeviceIdType.MESH
NX = 4
COLORS = 3
SLOTS = 3
CHUNKS = 8
ORDERS = (("x", "y", "z"), ("y", "z", "x"), ("z", "x", "y"))
STEP = {"x": 1, "y": 4, "z": 16}
F32, BF16 = jnp.float32, jnp.bfloat16


def coords(me):
    return {"x": lax.rem(me, 4), "y": lax.rem(lax.div(me, 4), 4), "z": lax.div(me, 16)}


def shifted(me, pos, axis, d):
    there = lax.rem(pos[axis] + d, 4)
    return me + (there - pos[axis]) * STEP[axis]


def remote(src, dst, send, recv, device):
    return pltpu.make_async_remote_copy(src_ref=src, dst_ref=dst, send_sem=send, recv_sem=recv, device_id=device, device_id_type=MESH)


def greet(devices):
    barrier = pltpu.get_barrier_semaphore()
    for n in devices:
        pl.semaphore_signal(barrier, inc=1, device_id=n, device_id_type=MESH)
    pl.semaphore_wait(barrier, len(devices))


def grad_kernel(total_tokens, emb_scale, u_ref, table_ref, xt_ref, ids_ref, stat_ref, h_ref, gain_ref, loss_ref,
                grad_ref, dh_ref, small_ref, own, buf2, buf3, ra0, ra1, ra2, rb, rc, ubuf, tbuf, dz, dxn, dxn_in, sums, sums_in,
                load_sem, ssem, rsem, xsend, xrecv, sum_send, sum_recv, credit):
    me = lax.axis_index("fsdp")
    tp = lax.axis_index("tp")
    pos = coords(me)
    chunks = CHUNKS
    lanes = own.shape[-1]
    rows = own.shape[-2]
    tokens, width = h_ref.shape
    vocab = u_ref.shape[1]
    quarter = vocab // NX
    ra = (ra0, ra1, ra2)
    near = [{"fsdp": shifted(me, pos, a, d)} for a in "xyz" for d in (1, 3)]
    partner = {"tp": 1 - tp}
    greet(near + [{"fsdp": shifted(me, pos, a, 2)} for a in "xyz"] + [partner])

    def loads(i):
        c, q = lax.div(i, NX), lax.rem(i, NX)
        s = lax.rem(i, 2)
        at = pl.ds(pl.multiple_of(q * quarter + c * lanes, 128), lanes)
        return (pltpu.make_async_copy(u_ref.at[:, at], ubuf.at[s], load_sem.at[s, 0]),
                pltpu.make_async_copy(table_ref.at[:, at], tbuf.at[s], load_sem.at[s, 1]))

    def produce(c, slot):
        def one(q, carry):
            i = c * NX + q
            s = lax.rem(i, 2)
            for cp in loads(i):
                cp.wait()

            @pl.when(i + 1 < chunks * NX)
            def _():
                for cp in loads(i + 1):
                    cp.start()

            first_id = q * quarter + c * lanes

            def block(b, carry):
                r = pl.ds(pl.multiple_of(b * 256, 256), 256)
                ids = lax.broadcasted_iota(jnp.int32, (256, lanes), 1) + first_id
                u = ubuf[s, r]
                prob = jnp.exp(SOFT_CAP * u - stat_ref[r, 0:1])
                hit = (ids_ref[r, 1:2] == ids).astype(F32)
                d = ((prob - hit) * (1.0 - u * u) / total_tokens).astype(BF16)
                dz[r] = d
                dz[pl.ds(pl.multiple_of(tokens + b * 256, 256), 256)] = jnp.where(ids_ref[r, 0:1] == ids, emb_scale, 0.0).astype(BF16)
                part = lax.dot_general(d, tbuf[s], (((1,), (1,)), ((), ())), preferred_element_type=F32)
                dxn[r] = dxn[r] + part
                return carry

            lax.fori_loop(0, tokens // 256, block, 0)

            def out(z, carry):
                w = width // 4
                v = jnp.dot(xt_ref[pl.ds(pl.multiple_of(z * w, 32), w), :], dz[...], preferred_element_type=F32)
                own[slot, q, z] = v.reshape(4, COLORS, rows, lanes)
                return carry

            lax.fori_loop(0, 4, out, 0)
            return carry

        lax.fori_loop(0, NX, one, 0)

    def own_at(s, k, a1, half):
        o = ORDERS[k]
        sel = {o[0]: a1, o[1]: pl.ds(2 * half, 2), o[2]: slice(None)}
        return own.at[s, sel["x"], sel["z"], sel["y"], k]

    def part(phase, k, s, a, half):
        if phase == 0:
            return own_at(s, k, a, half)
        if phase == 1:
            return buf2.at[s, k, a, pl.ds(2 * half, 2)]
        return buf3.at[s, k, a, :, pl.ds(128 * half, 128)]

    def land(phase, k, s, m):
        return ra[k].at[s, m] if phase == 0 else (rb, rc)[phase - 1].at[s, k, m]

    def copies(phase, k, s, step):
        axis = ORDERS[k][phase]
        p = pos[axis]
        right, left, far = lax.rem(p + 1, 4), lax.rem(p + 3, 4), lax.rem(p + 2, 4)
        to_r, to_l = {"fsdp": shifted(me, pos, axis, 1)}, {"fsdp": shifted(me, pos, axis, 3)}
        if step == 0:
            table = ((0, part(phase, k, s, far, 0), to_r), (1, part(phase, k, s, far, 1), to_l),
                     (2, part(phase, k, s, right, 1), to_r), (3, part(phase, k, s, left, 0), to_l))
        else:
            table = ((4, land(phase, k, s, 0), to_r), (5, land(phase, k, s, 1), to_l))
        return [(m, remote(src, land(phase, k, s, m), ssem.at[phase, s, k, m], rsem.at[phase, s, k, m], dev)) for m, src, dev in table]

    def first(phase, s):
        for k in range(COLORS):
            for _, cp in copies(phase, k, s, 0):
                cp.start()

    def second(phase, s):
        for k in range(COLORS):
            axis = ORDERS[k][phase]
            p = pos[axis]
            right, left = lax.rem(p + 1, 4), lax.rem(p + 3, 4)
            one = copies(phase, k, s, 0)
            for m, a in ((0, right), (1, left)):
                one[m][1].wait_recv()
                dst = land(phase, k, s, m)
                dst[...] = dst[...] + part(phase, k, s, a, m)[...]
            for _, cp in copies(phase, k, s, 1):
                cp.start()

    def last(phase, s, store):
        for k in range(COLORS):
            p = pos[ORDERS[k][phase]]
            one, two = copies(phase, k, s, 0), copies(phase, k, s, 1)
            for m, cp in one[2:] + two:
                cp.wait_recv()
            for half, (m, n) in enumerate(((4, 3), (5, 2))):
                store(k, half, part(phase, k, s, p, half)[...] + land(phase, k, s, m)[...] + land(phase, k, s, n)[...])
            for m, cp in one + two:
                cp.wait_send()

    def store1(s):
        def put(k, half, v):
            if k == 2:
                for i in range(2):
                    buf2[s, k, 2 * half + i] = v[i]
            else:
                for i in range(2):
                    buf2[s, k, 2 * half + i] = v[:, i]
        return put

    def store2(s):
        def put(k, half, v):
            buf3[s, k, pl.ds(2 * half, 2)] = v
        return put

    def store3(c):
        def put(k, half, v):
            grad_ref[k, :, pl.ds(pl.multiple_of(c * lanes + 128 * half, 128), 128)] = v
        return put

    half_rows = tokens // 2
    mine = pl.ds(pl.multiple_of(tp * half_rows, half_rows), half_rows)
    other = pl.ds(pl.multiple_of((1 - tp) * half_rows, half_rows), half_rows)

    def swap_dxn():
        return remote(dxn.at[other], dxn_in, xsend.at[0], xrecv.at[0], partner)

    def swap_dh():
        return remote(dh_ref.at[mine], dh_ref.at[mine], xsend.at[1], xrecv.at[1], partner)

    def finish_hidden():
        swap_dxn().wait()
        sums[...] = jnp.zeros_like(sums)
        gain = gain_ref[...]

        def block(b, acc):
            lo = pl.ds(pl.multiple_of(b * 128, 128), 128)
            r = pl.ds(pl.multiple_of(tp * half_rows + b * 128, 128), 128)
            inv = stat_ref[r, 1:2]
            hn = h_ref[r].astype(F32) * inv
            dx = dxn[r] + dxn_in[lo]
            g_dir = dx * gain
            mean = jnp.mean(g_dir * hn, axis=1, keepdims=True)
            dh_ref[r] = (inv * (g_dir - hn * mean)).astype(BF16)
            return acc + jnp.sum(dx * hn, axis=0, keepdims=True)

        dg = lax.fori_loop(0, half_rows // 128, block, jnp.zeros((1, width), F32))
        n = width // 128
        for i in range(n):
            sums[pl.ds(i, 1), :] = dg[:, 128 * i:128 * i + 128]
        sums[pl.ds(n, 1), :] = loss_ref[...]
        swap_dh().start()

    def sum_copies(phase):
        if phase == 3:
            peers = [partner]
        else:
            peers = [{"fsdp": shifted(me, pos, "xyz"[phase], d)} for d in (1, 2, 3)]
        return [remote(sums, sums_in.at[phase, j], sum_send.at[phase, j], sum_recv.at[phase, j], n) for j, n in enumerate(peers)]

    def sum_start(phase):
        for cp in sum_copies(phase):
            cp.start()

    def sum_end(phase):
        cps = sum_copies(phase)
        for cp in cps:
            cp.wait()
        if phase == 3:
            small_ref[...] = sums[...] + sums_in[3, 0]
        else:
            sums[...] = sums[...] + sums_in[phase, 0] + sums_in[phase, 1] + sums_in[phase, 2]

    dxn[...] = jnp.zeros_like(dxn)
    for cp in loads(0):
        cp.start()
    ticks = chunks + 6

    def tick(t, carry):
        @pl.when(t < chunks)
        def _():
            produce(t, lax.rem(t, SLOTS))

        @pl.when(t >= 1)
        def _():
            for i in range(6):
                pl.semaphore_wait(credit.at[i], 1)

        def stage(delay, run):
            c = t - delay
            @pl.when(jnp.logical_and(c >= 0, c < chunks))
            def _():
                run(c, lax.rem(c, SLOTS))

        def s2(c, s):
            last(0, s, store1(s))
            first(1, s)

        def s4(c, s):
            last(1, s, store2(s))
            first(2, s)

        stage(0, lambda c, s: first(0, s))
        @pl.when(t == chunks - 1)
        def _():
            swap_dxn().start()
        stage(6, lambda c, s: last(2, s, store3(c)))
        stage(5, lambda c, s: second(2, s))
        stage(4, s4)
        stage(3, lambda c, s: second(1, s))
        stage(2, s2)
        stage(1, lambda c, s: second(0, s))

        @pl.when(t == chunks)
        def _():
            finish_hidden()
        @pl.when(t == chunks + 1)
        def _():
            sum_start(0)
            swap_dh().wait()
        for phase in range(3):
            @pl.when(t == chunks + 2 + phase)
            def _():
                sum_end(phase)
                sum_start(phase + 1)
        @pl.when(t == chunks + 5)
        def _():
            sum_end(3)

        @pl.when(t < ticks - 1)
        def _():
            for i, n in enumerate(near):
                pl.semaphore_signal(credit.at[i], inc=1, device_id=n, device_id_type=MESH)
        return carry

    lax.fori_loop(0, ticks, tick, 0)


def gradients(total_tokens, emb_scale, u, table, xt, ids, stat, h, gain, loss):
    tokens, vocab = u.shape
    width = h.shape[1]
    quarter = vocab // NX
    lanes = quarter // CHUNKS
    rows = width // 48
    vm = pl.BlockSpec(memory_space=pltpu.VMEM)
    hbm = pl.BlockSpec(memory_space=pl.ANY)
    dma = pltpu.SemaphoreType.DMA
    return pl.pallas_call(
        functools.partial(grad_kernel, total_tokens, emb_scale),
        out_shape=[jax.ShapeDtypeStruct((COLORS, rows, quarter), F32), jax.ShapeDtypeStruct((tokens, width), BF16), jax.ShapeDtypeStruct((16, 128), F32)],
        in_specs=[hbm, hbm] + [vm] * 6,
        out_specs=[vm, vm, vm],
        scratch_shapes=[
            pltpu.VMEM((SLOTS, 4, 4, 4, COLORS, rows, lanes), F32),
            pltpu.VMEM((SLOTS, COLORS, 4, 4, rows, lanes), F32),
            pltpu.VMEM((SLOTS, COLORS, 4, rows, lanes), F32),
            pltpu.VMEM((SLOTS, 6, 4, 2, rows, lanes), F32),
            pltpu.VMEM((SLOTS, 6, 4, 2, rows, lanes), F32),
            pltpu.VMEM((SLOTS, 6, 2, 4, rows, lanes), F32),
            pltpu.VMEM((SLOTS, COLORS, 6, 2, rows, lanes), F32),
            pltpu.VMEM((SLOTS, COLORS, 6, rows, 128), F32),
            pltpu.VMEM((2, tokens, lanes), F32),
            pltpu.VMEM((2, width, lanes), BF16),
            pltpu.VMEM((2 * tokens, lanes), BF16),
            pltpu.VMEM((tokens, width), F32),
            pltpu.VMEM((tokens // 2, width), F32),
            pltpu.VMEM((16, 128), F32),
            pltpu.VMEM((4, 3, 16, 128), F32),
            dma((2, 2)),
            dma((3, SLOTS, COLORS, 6)),
            dma((3, SLOTS, COLORS, 6)),
            dma((2,)),
            dma((2,)),
            dma((4, 3)),
            dma((4, 3)),
            pltpu.SemaphoreType.REGULAR((6,)),
        ],
        compiler_params=pltpu.CompilerParams(collective_id=2, has_side_effects=True, vmem_limit_bytes=63 * 2**20),
    )(u, table, xt, ids, stat, h, gain, loss)


def math_scale(width):
    import numpy as np
    return float(np.asarray(math.sqrt(width), BF16).astype(np.float32))


def solution(mesh):
    fsdp_size = mesh.shape["fsdp"]
    groups = fsdp_size // NX
    x_groups = [[i * NX + j for j in range(NX)] for i in range(groups)]

    def device_step(emb_shard, tok_ids, lab_ids, h_last, g_embed, norm_w):
        vocab_rows, cols = emb_shard.shape
        batch_loc, seq_len, width = h_last.shape
        tok_count = batch_loc * seq_len
        total_tokens = tok_count * fsdp_size
        quarter = vocab_rows // NX
        row_start = lax.axis_index("tp") * vocab_rows
        me = lax.axis_index("fsdp")
        vocab_iota = jnp.arange(vocab_rows, dtype=jnp.int32)
        emb_scale = jnp.asarray(math.sqrt(width), jnp.bfloat16).astype(jnp.float32)

        piece = emb_shard.T.astype(jnp.bfloat16).reshape(cols, NX, quarter).transpose(1, 0, 2)
        piece = lax.all_to_all(piece, "fsdp", split_axis=0, concat_axis=0, axis_index_groups=x_groups)
        piece = piece.reshape(NX * cols, quarter)
        table = lax.all_gather(piece, "fsdp", axis=0)
        table = table.reshape(groups, NX, NX * cols, quarter).transpose(0, 2, 1, 3).reshape(width, vocab_rows)

        tok_local = tok_ids.reshape(tok_count) - row_start
        tok_hit = (tok_local[:, None] == vocab_iota[None, :]).astype(jnp.bfloat16)
        row_vals = jnp.einsum("tv,dv->td", tok_hit, table, preferred_element_type=jnp.float32).astype(jnp.bfloat16)
        row_vals = lax.psum(row_vals, "tp")
        x_emb = (row_vals.astype(jnp.float32) * emb_scale).astype(jnp.bfloat16)

        mine = jnp.where(lax.axis_index("tp") == 0, norm_w, 0.0)
        norm_full = lax.dynamic_update_slice(jnp.zeros((width,), jnp.float32), mine, (me * cols,))
        norm_gain = 1.0 + lax.psum(norm_full, ("tp", "fsdp"))
        h_wide = h_last.reshape(tok_count, width).astype(jnp.float32)
        inv_rms = lax.rsqrt(jnp.mean(h_wide * h_wide, axis=1, keepdims=True) + NORM_EPS)
        h_norm = h_wide * inv_rms
        x_norm = (h_norm * norm_gain).astype(jnp.bfloat16)

        logits = jnp.einsum("td,dv->tv", x_norm, table, preferred_element_type=jnp.float32)
        tanh_z = jnp.tanh(logits / SOFT_CAP)
        capped = SOFT_CAP * tanh_z
        exp_shift = jnp.exp(capped - SOFT_CAP)
        lab_hit = (lab_ids.reshape(tok_count) - row_start)[:, None] == vocab_iota[None, :]
        tok_stats = jnp.stack([jnp.sum(exp_shift, axis=1), jnp.sum(jnp.where(lab_hit, capped, 0.0), axis=1)])
        tok_stats = lax.psum(tok_stats, "tp")
        sum_exp = tok_stats[0]
        log_norm = jnp.log(sum_exp) + SOFT_CAP
        loss_part = 0.5 * jnp.sum(log_norm - tok_stats[1])

        xt = jnp.concatenate([x_norm.T, g_embed.reshape(tok_count, width).T], axis=1)
        ids = jnp.stack([tok_local, lab_ids.reshape(tok_count) - row_start], axis=1)
        stat = jnp.concatenate([log_norm[:, None], inv_rms], axis=1)
        grad, d_hidden, small = gradients(total_tokens, math_scale(width), tanh_z, table, xt, ids, stat, h_last.reshape(tok_count, width), norm_gain[None, :], jnp.full((1, 128), loss_part))
        loss_val = small[width // 128, 0] / total_tokens
        d_norm_w = lax.dynamic_slice(small.reshape(-1), (me * cols,), (cols,))
        grad = lax.all_to_all(grad.reshape(NX, cols, quarter), "fsdp", split_axis=0, concat_axis=0, axis_index_groups=x_groups)
        d_table = grad.transpose(1, 0, 2).reshape(cols, vocab_rows).T
        return (x_emb.reshape(batch_loc, seq_len, width), loss_val, d_hidden.reshape(batch_loc, seq_len, width), d_norm_w, d_table)

    spec_tok = P("fsdp", None)
    spec_act = P("fsdp", None, None)
    return jax.shard_map(device_step, mesh=mesh, in_specs=(P("tp", "fsdp"), spec_tok, spec_tok, spec_act, spec_act, P("fsdp")), out_specs=(spec_act, P(), spec_act, P("fsdp"), P("tp", "fsdp")), check_vma=False)
```

```python
import functools
import math
import jax
import jax.numpy as jnp
from jax import lax
from jax.experimental import pallas as pl
from jax.experimental.pallas import tpu as pltpu
from jax.sharding import PartitionSpec as P

SOFT_CAP = 30.0
NORM_EPS = 1e-6
MESH = pl.DeviceIdType.MESH
NX = 4
COLORS = 3
SLOTS = 3
CHUNKS = 8
ORDERS = (("x", "y", "z"), ("y", "z", "x"), ("z", "x", "y"))
STEP = {"x": 1, "y": 4, "z": 16}
LANE = 128
ROWS = 256
F32, BF16 = jnp.float32, jnp.bfloat16


def coords(me):
    return {"x": lax.rem(me, 4), "y": lax.rem(lax.div(me, 4), 4), "z": lax.div(me, 16)}


def shifted(me, pos, axis, d):
    there = lax.rem(pos[axis] + d, 4)
    return me + (there - pos[axis]) * STEP[axis]


def span(start, size):
    return pl.ds(pl.multiple_of(start, size), size)


def remote(src, dst, send, recv, device):
    return pltpu.make_async_remote_copy(src_ref=src, dst_ref=dst, send_sem=send, recv_sem=recv, device_id=device, device_id_type=MESH)


def greet(devices):
    barrier = pltpu.get_barrier_semaphore()
    for n in devices:
        pl.semaphore_signal(barrier, inc=1, device_id=n, device_id_type=MESH)
    pl.semaphore_wait(barrier, len(devices))


def grad_kernel(total_tokens, emb_scale, u_ref, table_ref, xt_ref, ids_ref, stat_ref, h_ref, gain_ref, loss_ref,
                grad_ref, dh_ref, small_ref, look_ref, own, buf2, buf3, ra0, ra1, ra2, rb, rc, ubuf, tbuf, dz, dxn, dxn_in, look_in, sums, sums_in,
                load_sem, ssem, rsem, xsend, xrecv, sum_send, sum_recv, credit, look_free):
    me = lax.axis_index("fsdp")
    tp = lax.axis_index("tp")
    pos = coords(me)
    chunks = CHUNKS
    lanes = own.shape[-1]
    rows = own.shape[-2]
    tokens, width = h_ref.shape
    vocab = u_ref.shape[1]
    quarter = vocab // NX
    ra = (ra0, ra1, ra2)
    near = [{"fsdp": shifted(me, pos, a, d)} for a in "xyz" for d in (1, 3)]
    partner = {"tp": 1 - tp}
    greet(near + [{"fsdp": shifted(me, pos, a, 2)} for a in "xyz"] + [partner])

    def loads(i):
        c, q = lax.div(i, NX), lax.rem(i, NX)
        s = lax.rem(i, 2)
        at = pl.ds(pl.multiple_of(q * quarter + c * lanes, LANE), lanes)
        return (pltpu.make_async_copy(u_ref.at[:, at], ubuf.at[s], load_sem.at[s, 0]),
                pltpu.make_async_copy(table_ref.at[:, at], tbuf.at[s], load_sem.at[s, 1]))

    def produce(c, slot):
        def one(q, carry):
            i = c * NX + q
            s = lax.rem(i, 2)
            for cp in loads(i):
                cp.wait()

            @pl.when(i + 1 < chunks * NX)
            def _():
                for cp in loads(i + 1):
                    cp.start()

            first_id = q * quarter + c * lanes

            def block(b, carry):
                r = span(b * ROWS, ROWS)
                ids = lax.broadcasted_iota(jnp.int32, (ROWS, lanes), 1) + first_id
                u = ubuf[s, r]
                prob = jnp.exp(SOFT_CAP * u - stat_ref[r, 0:1])
                hit = (ids_ref[r, 1:2] == ids).astype(F32)
                d = ((prob - hit) * (1.0 - u * u) / total_tokens).astype(BF16)
                dz[r] = d
                pick = jnp.where(ids_ref[r, 0:1] == ids, emb_scale, 0.0).astype(BF16)
                dz[pl.ds(pl.multiple_of(tokens + b * ROWS, ROWS), ROWS)] = pick
                part = lax.dot_general(d, tbuf[s], (((1,), (1,)), ((), ())), preferred_element_type=F32)
                dxn[r] = dxn[r] + part
                found = lax.dot_general(pick, tbuf[s], (((1,), (1,)), ((), ())), preferred_element_type=F32)
                look_ref[r] = look_ref[r] + found.astype(BF16)
                return carry

            lax.fori_loop(0, tokens // ROWS, block, 0, unroll=True)

            def out(z, carry):
                w = width // 4
                v = jnp.dot(xt_ref[pl.ds(pl.multiple_of(z * w, 32), w), :], dz[...], preferred_element_type=F32)
                own[slot, q, z] = v.reshape(4, COLORS, rows, lanes)
                return carry

            lax.fori_loop(0, 4, out, 0, unroll=True)
            return carry

        lax.fori_loop(0, NX, one, 0)

    def own_at(s, k, a1, half):
        o = ORDERS[k]
        sel = {o[0]: a1, o[1]: pl.ds(2 * half, 2), o[2]: slice(None)}
        return own.at[s, sel["x"], sel["z"], sel["y"], k]

    def part(phase, k, s, a, half):
        if phase == 0:
            return own_at(s, k, a, half)
        if phase == 1:
            return buf2.at[s, k, a, pl.ds(2 * half, 2)]
        return buf3.at[s, k, a, :, pl.ds(LANE * half, LANE)]

    def land(phase, k, s, m):
        return ra[k].at[s, m] if phase == 0 else (rb, rc)[phase - 1].at[s, k, m]

    def copies(phase, k, s, step):
        axis = ORDERS[k][phase]
        p = pos[axis]
        right, left, far = lax.rem(p + 1, 4), lax.rem(p + 3, 4), lax.rem(p + 2, 4)
        to_r, to_l = {"fsdp": shifted(me, pos, axis, 1)}, {"fsdp": shifted(me, pos, axis, 3)}
        if step == 0:
            table = ((0, part(phase, k, s, far, 0), to_r), (1, part(phase, k, s, far, 1), to_l),
                     (2, part(phase, k, s, right, 1), to_r), (3, part(phase, k, s, left, 0), to_l))
        else:
            table = ((4, land(phase, k, s, 0), to_r), (5, land(phase, k, s, 1), to_l))
        return [(m, remote(src, land(phase, k, s, m), ssem.at[phase, s, k, m], rsem.at[phase, s, k, m], dev)) for m, src, dev in table]

    def first(phase, s):
        for k in range(COLORS):
            for _, cp in copies(phase, k, s, 0):
                cp.start()

    def second(phase, s):
        for k in range(COLORS):
            axis = ORDERS[k][phase]
            p = pos[axis]
            right, left = lax.rem(p + 1, 4), lax.rem(p + 3, 4)
            one = copies(phase, k, s, 0)
            for m, a in ((0, right), (1, left)):
                one[m][1].wait_recv()
                dst = land(phase, k, s, m)
                dst[...] = dst[...] + part(phase, k, s, a, m)[...]
            for _, cp in copies(phase, k, s, 1):
                cp.start()

    def last(phase, s, store):
        for k in range(COLORS):
            p = pos[ORDERS[k][phase]]
            one, two = copies(phase, k, s, 0), copies(phase, k, s, 1)
            for m, cp in one[2:] + two:
                cp.wait_recv()
            for half, (m, n) in enumerate(((4, 3), (5, 2))):
                store(k, half, part(phase, k, s, p, half)[...] + land(phase, k, s, m)[...] + land(phase, k, s, n)[...])
            for m, cp in one + two:
                cp.wait_send()

    def store1(s):
        def put(k, half, v):
            if k == 2:
                for i in range(2):
                    buf2[s, k, 2 * half + i] = v[i]
            else:
                for i in range(2):
                    buf2[s, k, 2 * half + i] = v[:, i]
        return put

    def store2(s):
        def put(k, half, v):
            buf3[s, k, pl.ds(2 * half, 2)] = v
        return put

    def store3(c):
        def put(k, half, v):
            grad_ref[k, :, pl.ds(pl.multiple_of(c * lanes + LANE * half, LANE), LANE)] = v
        return put

    half_rows = tokens // 2
    mine = pl.ds(pl.multiple_of(tp * half_rows, half_rows), half_rows)
    other = pl.ds(pl.multiple_of((1 - tp) * half_rows, half_rows), half_rows)

    def swap_dxn():
        return remote(dxn.at[other], dxn_in, xsend.at[0], xrecv.at[0], partner)

    def swap_dh():
        return remote(dh_ref.at[mine], dh_ref.at[mine], xsend.at[1], xrecv.at[1], partner)

    def swap_look(back):
        if back:
            return remote(look_ref.at[mine], look_ref.at[mine], xsend.at[3], xrecv.at[3], partner)
        return remote(look_ref.at[other], look_in, xsend.at[2], xrecv.at[2], partner)

    def finish_look():
        swap_look(False).wait()
        pl.semaphore_signal(look_free, inc=1, device_id=partner, device_id_type=MESH)
        look_ref[mine] = look_ref[mine] + look_in[...]

    def finish_hidden():
        swap_dxn().wait()
        sums[...] = jnp.zeros_like(sums)
        gain = gain_ref[...]

        def block(b, acc):
            lo = span(b * LANE, LANE)
            r = span(tp * half_rows + b * LANE, LANE)
            inv = stat_ref[r, 1:2]
            hn = h_ref[r].astype(F32) * inv
            dx = dxn[r] + dxn_in[lo]
            g_dir = dx * gain
            mean = jnp.mean(g_dir * hn, axis=1, keepdims=True)
            dh_ref[r] = (inv * (g_dir - hn * mean)).astype(BF16)
            return acc + jnp.sum(dx * hn, axis=0, keepdims=True)

        dg = lax.fori_loop(0, half_rows // LANE, block, jnp.zeros((1, width), F32))
        n = width // LANE
        for i in range(n):
            sums[pl.ds(i, 1), :] = dg[:, LANE * i:LANE * i + LANE]
        sums[pl.ds(n, 1), :] = loss_ref[...]
        swap_dh().start()

    def sum_copies(phase):
        if phase == 3:
            peers = [partner]
        else:
            peers = [{"fsdp": shifted(me, pos, "xyz"[phase], d)} for d in (1, 2, 3)]
        return [remote(sums, sums_in.at[phase, j], sum_send.at[phase, j], sum_recv.at[phase, j], n) for j, n in enumerate(peers)]

    def sum_start(phase):
        for cp in sum_copies(phase):
            cp.start()

    def sum_end(phase):
        cps = sum_copies(phase)
        for cp in cps:
            cp.wait()
        if phase == 3:
            small_ref[...] = sums[...] + sums_in[3, 0]
        else:
            sums[...] = sums[...] + sums_in[phase, 0] + sums_in[phase, 1] + sums_in[phase, 2]

    dxn[...] = jnp.zeros_like(dxn)
    look_ref[...] = jnp.zeros_like(look_ref)
    for cp in loads(0):
        cp.start()
    ticks = chunks + 6

    def tick(t, carry):
        @pl.when(t < chunks)
        def _():
            produce(t, lax.rem(t, SLOTS))

        @pl.when(t >= 1)
        def _():
            for i in range(6):
                pl.semaphore_wait(credit.at[i], 1)

        def stage(delay, run):
            c = t - delay
            @pl.when(jnp.logical_and(c >= 0, c < chunks))
            def _():
                run(c, lax.rem(c, SLOTS))

        def s2(c, s):
            last(0, s, store1(s))
            first(1, s)

        def s4(c, s):
            last(1, s, store2(s))
            first(2, s)

        stage(0, lambda c, s: first(0, s))
        @pl.when(t == chunks - 1)
        def _():
            swap_dxn().start()
            swap_look(False).start()
        stage(6, lambda c, s: last(2, s, store3(c)))
        stage(5, lambda c, s: second(2, s))
        stage(4, s4)
        stage(3, lambda c, s: second(1, s))
        stage(2, s2)
        stage(1, lambda c, s: second(0, s))

        @pl.when(t == chunks)
        def _():
            finish_hidden()
        @pl.when(t == chunks + 1)
        def _():
            sum_start(0)
            swap_dh().wait()
            finish_look()
        for phase in range(3):
            @pl.when(t == chunks + 2 + phase)
            def _():
                if phase == 0:
                    pl.semaphore_wait(look_free, 1)
                    swap_look(True).start()
                if phase == 2:
                    swap_look(True).wait()
                sum_end(phase)
                sum_start(phase + 1)
        @pl.when(t == chunks + 5)
        def _():
            sum_end(3)

        @pl.when(t < ticks - 1)
        def _():
            for i, n in enumerate(near):
                pl.semaphore_signal(credit.at[i], inc=1, device_id=n, device_id_type=MESH)
        return carry

    lax.fori_loop(0, ticks, tick, 0)


def gradients(total_tokens, emb_scale, u, table, xt, ids, stat, h, gain, loss):
    tokens, vocab = u.shape
    width = h.shape[1]
    quarter = vocab // NX
    lanes = quarter // CHUNKS
    rows = width // 48
    vm = pl.BlockSpec(memory_space=pltpu.VMEM)
    hbm = pl.BlockSpec(memory_space=pl.ANY)
    dma = pltpu.SemaphoreType.DMA
    return pl.pallas_call(
        functools.partial(grad_kernel, total_tokens, emb_scale),
        out_shape=[jax.ShapeDtypeStruct((COLORS, rows, quarter), F32), jax.ShapeDtypeStruct((tokens, width), BF16), jax.ShapeDtypeStruct((16, LANE), F32), jax.ShapeDtypeStruct((tokens, width), BF16)],
        in_specs=[hbm, hbm] + [vm] * 6,
        out_specs=[vm, vm, vm, vm],
        scratch_shapes=[
            pltpu.VMEM((SLOTS, 4, 4, 4, COLORS, rows, lanes), F32),
            pltpu.VMEM((SLOTS, COLORS, 4, 4, rows, lanes), F32),
            pltpu.VMEM((SLOTS, COLORS, 4, rows, lanes), F32),
            pltpu.VMEM((SLOTS, 6, 4, 2, rows, lanes), F32),
            pltpu.VMEM((SLOTS, 6, 4, 2, rows, lanes), F32),
            pltpu.VMEM((SLOTS, 6, 2, 4, rows, lanes), F32),
            pltpu.VMEM((SLOTS, COLORS, 6, 2, rows, lanes), F32),
            pltpu.VMEM((SLOTS, COLORS, 6, rows, LANE), F32),
            pltpu.VMEM((2, tokens, lanes), F32),
            pltpu.VMEM((2, width, lanes), BF16),
            pltpu.VMEM((2 * tokens, lanes), BF16),
            pltpu.VMEM((tokens, width), F32),
            pltpu.VMEM((tokens // 2, width), F32),
            pltpu.VMEM((tokens // 2, width), BF16),
            pltpu.VMEM((16, LANE), F32),
            pltpu.VMEM((4, 3, 16, LANE), F32),
            dma((2, 2)),
            dma((3, SLOTS, COLORS, 6)),
            dma((3, SLOTS, COLORS, 6)),
            dma((4,)),
            dma((4,)),
            dma((4, 3)),
            dma((4, 3)),
            pltpu.SemaphoreType.REGULAR((6,)),
            pltpu.SemaphoreType.REGULAR,
        ],
        compiler_params=pltpu.CompilerParams(collective_id=2, has_side_effects=True, vmem_limit_bytes=63 * 2**20),
    )(u, table, xt, ids, stat, h, gain, loss)


def table_kernel(emb_ref, norm_ref, h_ref, g_ref, ids_ref, u_ref, table_ref, xt_ref, stat_ref, gain_ref, loss_ref,
                 xin, mid, yin, tab, norms, norms_in, xn, rhs, ubuf, acc, sums, sums_in,
                 ex_send, ex_recv, nsend, nrecv, ssem, rsem, psend, precv, usem, tsem):
    me = lax.axis_index("fsdp")
    tp = lax.axis_index("tp")
    pos = coords(me)
    tokens, width = h_ref.shape
    parts, block, lanes = tab.shape[0], tab.shape[5], tab.shape[6]
    quarter = emb_ref.shape[2]
    cols = emb_ref.shape[1]
    sub = quarter // 4
    peers = {a: [{"fsdp": shifted(me, pos, a, d)} for d in (1, 2, 3)] for a in "xyz"}
    partner = {"tp": 1 - tp}
    greet(peers["x"] + peers["y"] + peers["z"] + [partner])

    def exchange(j):
        axis = "xy"[j]
        out = []
        for d in (1, 2, 3):
            there = lax.rem(pos[axis] + d, 4)
            src, dst = (emb_ref.at[there], xin.at[pos[axis]]) if j == 0 else (mid.at[there], yin.at[pos[axis]])
            out.append(remote(src, dst, ex_send.at[j, d - 1], ex_recv.at[j, d - 1], peers[axis][d - 1]))
        return out

    def norm_copies(j):
        return [remote(norms, norms_in.at[j, d], nsend.at[j, d], nrecv.at[j, d], peers["xyz"[j]][d]) for d in range(3)]

    def norm_start(j):
        for cp in norm_copies(j):
            cp.start()

    def norm_end(j):
        for cp in norm_copies(j):
            cp.wait()
        norms[...] = norms[...] + norms_in[j, 0] + norms_in[j, 1] + norms_in[j, 2]

    norms[...] = norm_ref[...]
    for cp in exchange(0):
        cp.start()
    xin[pos["x"]] = emb_ref[pos["x"]]
    norm_start(0)
    for cp in exchange(0):
        cp.wait()
    for j in range(4):
        for i in range(4):
            mid[j, pl.ds(cols * i, cols), :] = xin[i, :, pl.ds(sub * j, sub)]
    norm_end(0)
    norm_start(1)
    for cp in exchange(1):
        cp.start()
    yin[pos["y"]] = mid[pos["y"]]
    for cp in exchange(1):
        cp.wait()
    whole = jnp.concatenate([yin[i] for i in range(4)], axis=0).astype(BF16)
    for c in range(parts):
        for k in range(COLORS):
            tab[c, pos["x"], pos["y"], pos["z"], k] = whole[block * k:block * k + block, lanes * c:lanes * c + lanes]
    norm_end(1)
    norm_start(2)

    def region(e, kind, k, a, half):
        o = ORDERS[k]
        if kind == 0:
            sel = {o[0]: pos[o[0]], o[1]: pos[o[1]], o[2]: a}
            return tab.at[:, sel["x"], sel["y"], sel["z"], k, pl.ds(half * (block // 2), block // 2)]
        if kind == 1:
            sel = {o[0]: pos[o[0]], o[1]: a, o[2]: pl.ds(2 * half, 2)}
            return tab.at[:, sel["x"], sel["y"], sel["z"], k]
        sel = {o[0]: a, o[1]: pl.ds(2 * half, 2), o[2]: slice(None)}
        return tab.at[e - 2, sel["x"], sel["y"], sel["z"], k]

    def copies(e, k, step):
        kind = min(e, 2) if isinstance(e, int) else 2
        axis = ORDERS[k][2 - kind]
        p = pos[axis]
        right, left = lax.rem(p + 1, 4), lax.rem(p + 3, 4)
        to_r, to_l = {"fsdp": shifted(me, pos, axis, 1)}, {"fsdp": shifted(me, pos, axis, 3)}
        if step == 0:
            plan = ((0, p, 0, to_r), (1, p, 1, to_l), (2, p, 1, to_r), (3, p, 0, to_l))
        else:
            plan = ((4, left, 0, to_r), (5, right, 1, to_l))
        return [remote(region(e, kind, k, a, half), region(e, kind, k, a, half), ssem.at[e, k, m], rsem.at[e, k, m], dev)
                for m, a, half, dev in plan]

    def begin(e):
        for k in range(COLORS):
            for cp in copies(e, k, 0):
                cp.start()

    def forward(e):
        for k in range(COLORS):
            one, two = copies(e, k, 0), copies(e, k, 1)
            one[0].wait_recv()
            two[0].start()
            one[1].wait_recv()
            two[1].start()

    def arrive(e):
        for k in range(COLORS):
            one, two = copies(e, k, 0), copies(e, k, 1)
            for cp in one[2:] + two:
                cp.wait_recv()
            for cp in one + two:
                cp.wait_send()

    begin(0)
    forward(0)
    arrive(0)
    begin(1)
    norm_end(2)
    n = width // LANE
    gain = 1.0 + jnp.concatenate([norms[pl.ds(i, 1), :] for i in range(n)], axis=1)
    gain_ref[...] = gain

    def normalize(b, carry):
        r = span(b * LANE, LANE)
        hw = h_ref[r].astype(F32)
        inv = lax.rsqrt(jnp.mean(hw * hw, axis=1, keepdims=True) + NORM_EPS)
        v = (hw * inv * gain_ref[...]).astype(BF16)
        xn[r] = v
        stat_ref[r, 1:2] = inv
        xt_ref[:, r] = v.T
        xt_ref[:, span(tokens + b * LANE, LANE)] = g_ref[r].T
        return carry

    lax.fori_loop(0, tokens // LANE, normalize, 0)
    forward(1)
    acc[...] = jnp.zeros_like(acc)
    arrive(1)
    begin(2)

    def u_out(i):
        c, p = lax.div(i, 8), lax.rem(i, 8)
        s = lax.rem(i, 2)
        base = lax.div(p, 2) * quarter + lax.rem(p, 2) * (2 * sub) + c * lanes
        return [pltpu.make_async_copy(ubuf.at[s, j], u_ref.at[:, pl.ds(pl.multiple_of(base + j * sub, LANE), lanes)], usem.at[s, j]) for j in range(2)]

    def table_out(c):
        cps = []
        for x in range(4):
            for y in range(4):
                at = pl.ds(pl.multiple_of(x * quarter + y * sub + c * lanes, LANE), lanes)
                cps.append(pltpu.make_async_copy(tab.at[c, x, y], table_ref.at[:, :, :, at], tsem.at[x, y]))
        return cps

    def chunk(c, carry):
        forward(c + 2)

        @pl.when(c + 1 < parts)
        def _():
            begin(c + 3)

        arrive(c + 2)

        @pl.when(c >= 1)
        def _():
            for cp in table_out(c - 1):
                cp.wait()
        for cp in table_out(c):
            cp.start()

        def pair(p, carry):
            i = c * 8 + p
            s = lax.rem(i, 2)
            x, y = lax.div(p, 2), lax.rem(p, 2) * 2
            for j in range(2):
                rhs[:, lanes * j:lanes * j + lanes] = tab[c, x, y + j].reshape(width, lanes)

            @pl.when(i >= 2)
            def _():
                for cp in u_out(i - 2):
                    cp.wait()
            base = x * quarter + y * sub + c * lanes
            lane = lax.broadcasted_iota(jnp.int32, (ROWS, 2 * lanes), 1)
            ids = lane + base + jnp.where(lane >= lanes, sub - lanes, 0)

            def rows(b, carry):
                r = span(b * ROWS, ROWS)
                z = jnp.dot(xn[r], rhs[...], preferred_element_type=F32)
                u = jnp.tanh(z * (1.0 / SOFT_CAP))
                for j in range(2):
                    ubuf[s, j, r] = u[:, lanes * j:lanes * j + lanes]
                capped = SOFT_CAP * u
                e = jnp.exp(capped - SOFT_CAP)
                hit = jnp.where(ids_ref[r, 1:2] == ids, capped, 0.0)
                acc[0, r] = acc[0, r] + e[:, :lanes] + e[:, lanes:]
                acc[1, r] = acc[1, r] + hit[:, :lanes] + hit[:, lanes:]
                return carry

            lax.fori_loop(0, tokens // ROWS, rows, 0, unroll=True)
            for cp in u_out(i):
                cp.start()
            return carry

        lax.fori_loop(0, 8, pair, 0)
        return carry

    lax.fori_loop(0, parts, chunk, 0)
    lane = lax.broadcasted_iota(jnp.int32, (tokens, LANE), 1)
    sums[...] = jnp.where(lane == 0, jnp.sum(acc[0], axis=1, keepdims=True), jnp.sum(acc[1], axis=1, keepdims=True))
    swap = remote(sums, sums_in, psend, precv, partner)
    swap.start()
    for cp in u_out(parts * 8 - 2) + u_out(parts * 8 - 1) + table_out(parts - 1):
        cp.wait()
    swap.wait()
    both = sums[...] + sums_in[...]
    lse = jnp.log(both[:, 0:1]) + SOFT_CAP
    stat_ref[:, 0:1] = lse
    loss_ref[...] = jnp.broadcast_to(0.5 * jnp.sum(lse - both[:, 1:2], axis=0, keepdims=True), (1, LANE))


def table_pass(emb, norm, h, g, ids):
    tokens, width = h.shape
    quarter = emb.shape[2]
    cols = emb.shape[1]
    vocab = NX * quarter
    sub = quarter // 4
    block = width // 12
    parts = sub // LANE
    vm = pl.BlockSpec(memory_space=pltpu.VMEM)
    hbm = pl.BlockSpec(memory_space=pl.ANY)
    dma = pltpu.SemaphoreType.DMA
    u, table, xt, stat, gain, loss = pl.pallas_call(
        table_kernel,
        out_shape=[
            jax.ShapeDtypeStruct((tokens, vocab), F32),
            jax.ShapeDtypeStruct((4, COLORS, block, vocab), BF16),
            jax.ShapeDtypeStruct((width, 2 * tokens), BF16),
            jax.ShapeDtypeStruct((tokens, 2), F32),
            jax.ShapeDtypeStruct((1, width), F32),
            jax.ShapeDtypeStruct((1, LANE), F32),
        ],
        in_specs=[vm] * 5,
        out_specs=[hbm, hbm, vm, vm, vm, vm],
        scratch_shapes=[
            pltpu.VMEM((4, cols, quarter), F32),
            pltpu.VMEM((4, 4 * cols, sub), F32),
            pltpu.VMEM((4, 4 * cols, sub), F32),
            pltpu.VMEM((parts, 4, 4, 4, COLORS, block, LANE), BF16),
            pltpu.VMEM((16, LANE), F32),
            pltpu.VMEM((3, 3, 16, LANE), F32),
            pltpu.VMEM((tokens, width), BF16),
            pltpu.VMEM((width, ROWS), BF16),
            pltpu.VMEM((2, 2, tokens, LANE), F32),
            pltpu.VMEM((2, tokens, LANE), F32),
            pltpu.VMEM((tokens, LANE), F32),
            pltpu.VMEM((tokens, LANE), F32),
            dma((2, 3)),
            dma((2, 3)),
            dma((3, 3)),
            dma((3, 3)),
            dma((2 + parts, COLORS, 6)),
            dma((2 + parts, COLORS, 6)),
            dma,
            dma,
            dma((2, 2)),
            dma((4, 4)),
        ],
        compiler_params=pltpu.CompilerParams(collective_id=1, has_side_effects=True, vmem_limit_bytes=63 * 2**20),
    )(emb, norm, h, g, ids)
    return u, table.reshape(width, vocab), xt, stat, gain, loss


def math_scale(width):
    import numpy as np
    return float(np.asarray(math.sqrt(width), BF16).astype(np.float32))


def solution(mesh):
    fsdp_size = mesh.shape["fsdp"]
    x_groups = [[i * NX + j for j in range(NX)] for i in range(fsdp_size // NX)]

    def device_step(emb_shard, tok_ids, lab_ids, h_last, g_embed, norm_w):
        vocab_rows, cols = emb_shard.shape
        batch_loc, seq_len, width = h_last.shape
        tok_count = batch_loc * seq_len
        total_tokens = tok_count * fsdp_size
        quarter = vocab_rows // NX
        row_start = lax.axis_index("tp") * vocab_rows
        me = lax.axis_index("fsdp")

        emb = emb_shard.T.reshape(cols, NX, quarter).transpose(1, 0, 2)
        norm = lax.dynamic_update_slice(jnp.zeros((16 * LANE,), F32), norm_w, (me * cols,)).reshape(16, LANE)
        ids = jnp.stack([tok_ids.reshape(tok_count) - row_start, lab_ids.reshape(tok_count) - row_start], axis=1)
        h = h_last.reshape(tok_count, width)
        g = g_embed.reshape(tok_count, width)
        u, table, xt, stat, gain, loss = table_pass(emb, norm, h, g, ids)
        grad, d_hidden, small, x_emb = gradients(total_tokens, math_scale(width), u, table, xt, ids, stat, h, gain, loss)
        loss_val = small[width // LANE, 0] / total_tokens
        d_norm_w = lax.dynamic_slice(small.reshape(-1), (me * cols,), (cols,))
        grad = lax.all_to_all(grad.reshape(NX, cols, quarter), "fsdp", split_axis=0, concat_axis=0, axis_index_groups=x_groups)
        d_table = grad.transpose(1, 0, 2).reshape(cols, vocab_rows).T
        return (x_emb.reshape(batch_loc, seq_len, width), loss_val, d_hidden.reshape(batch_loc, seq_len, width), d_norm_w, d_table)

    spec_tok = P("fsdp", None)
    spec_act = P("fsdp", None, None)
    return jax.shard_map(device_step, mesh=mesh, in_specs=(P("tp", "fsdp"), spec_tok, spec_tok, spec_act, spec_act, P("fsdp")), out_specs=(spec_act, P(), spec_act, P("fsdp"), P("tp", "fsdp")), check_vma=False)
```

```python
import functools
import math
import jax
import jax.numpy as jnp
from jax import lax
from jax.experimental import pallas as pl
from jax.experimental.pallas import tpu as pltpu
from jax.sharding import PartitionSpec as P

SOFT_CAP = 30.0
NORM_EPS = 1e-6
MESH = pl.DeviceIdType.MESH
NX = 4
COLORS = 3
SLOTS = 3
CHUNKS = 8
ORDERS = (("x", "y", "z"), ("y", "z", "x"), ("z", "x", "y"))
STEP = {"x": 1, "y": 4, "z": 16}
LANE = 128
ROWS = 256
F32, BF16 = jnp.float32, jnp.bfloat16


def coords(me):
    return {"x": lax.rem(me, 4), "y": lax.rem(lax.div(me, 4), 4), "z": lax.div(me, 16)}


def shifted(me, pos, axis, d):
    there = lax.rem(pos[axis] + d, 4)
    return me + (there - pos[axis]) * STEP[axis]


def span(start, size):
    return pl.ds(pl.multiple_of(start, size), size)


def remote(src, dst, send, recv, device):
    return pltpu.make_async_remote_copy(src_ref=src, dst_ref=dst, send_sem=send, recv_sem=recv, device_id=device, device_id_type=MESH)


def greet(devices):
    barrier = pltpu.get_barrier_semaphore()
    for n in devices:
        pl.semaphore_signal(barrier, device_id=n, device_id_type=MESH)
    pl.semaphore_wait(barrier, len(devices))


def grad_kernel(total_tokens, emb_scale, u_ref, table_ref, xt_ref, ids_ref, stat_ref, h_ref, gain_ref, loss_ref,
                grad_ref, dh_ref, small_ref, look_ref, own, buf2, buf3, ra0, ra1, ra2, rb, rc, ubuf, tbuf, dz, dxn, dxn_in, look_in, piece, sums, sums_in,
                load_sem, ssem, rsem, xsend, xrecv, sum_send, sum_recv, psend, precv, credit, look_free):
    me = lax.axis_index("fsdp")
    tp = lax.axis_index("tp")
    pos = coords(me)
    chunks = CHUNKS
    lanes = own.shape[-1]
    rows = own.shape[-2]
    tokens, width = h_ref.shape
    vocab = u_ref.shape[1]
    cols = grad_ref.shape[0]
    quarter = vocab // NX
    ra = (ra0, ra1, ra2)
    near = [{"fsdp": shifted(me, pos, a, d)} for a in "xyz" for d in (1, 3)]
    partner = {"tp": 1 - tp}
    everyone = near + [{"fsdp": shifted(me, pos, a, 2)} for a in "xyz"] + [partner]
    barrier = pltpu.get_barrier_semaphore()
    for n in everyone:
        pl.semaphore_signal(barrier, device_id=n, device_id_type=MESH)

    def loads(i):
        c, q = lax.div(i, NX), lax.rem(i, NX)
        s = lax.rem(i, 2)
        at = pl.ds(pl.multiple_of(q * quarter + c * lanes, LANE), lanes)
        return (pltpu.make_async_copy(u_ref.at[:, at], ubuf.at[s], load_sem.at[s, 0]),
                pltpu.make_async_copy(table_ref.at[:, at], tbuf.at[s], load_sem.at[s, 1]))

    def produce(c, slot):
        def one(q, carry):
            i = c * NX + q
            s = lax.rem(i, 2)
            for cp in loads(i):
                cp.wait()

            @pl.when(i + 1 < chunks * NX)
            def _():
                for cp in loads(i + 1):
                    cp.start()

            first_id = q * quarter + c * lanes

            def block(b, carry):
                r = span(b * ROWS, ROWS)
                ids = lax.broadcasted_iota(jnp.int32, (ROWS, lanes), 1) + first_id
                u = ubuf[s, r]
                prob = jnp.exp(SOFT_CAP * u - stat_ref[r, 0:1])
                hit = (ids_ref[r, 1:2] == ids).astype(F32)
                d = ((prob - hit) * (1.0 - u * u) * (1.0 / total_tokens)).astype(BF16)
                dz[r] = d
                pick = jnp.where(ids_ref[r, 0:1] == ids, emb_scale, 0.0).astype(BF16)
                dz[pl.ds(pl.multiple_of(tokens + b * ROWS, ROWS), ROWS)] = pick
                part = lax.dot_general(d, tbuf[s], (((1,), (1,)), ((), ())), preferred_element_type=F32)
                dxn[r] = dxn[r] + part
                found = lax.dot_general(pick, tbuf[s], (((1,), (1,)), ((), ())), preferred_element_type=F32)
                look_ref[r] = look_ref[r] + found.astype(BF16)
                return carry

            lax.fori_loop(0, tokens // ROWS, block, 0, unroll=True)

            def out(z, carry):
                w = width // 2
                v = jnp.dot(xt_ref[pl.ds(pl.multiple_of(z * w, 32), w), :], dz[...], preferred_element_type=F32)
                own[slot, q, pl.ds(2 * z, 2)] = v.reshape(2, 4, COLORS, rows, lanes)
                return carry

            lax.fori_loop(0, 2, out, 0, unroll=True)
            return carry

        lax.fori_loop(0, NX, one, 0)

    def own_at(c, k, a1, half):
        o = ORDERS[k]
        sel = {o[0]: a1, o[1]: pl.ds(2 * half, 2), o[2]: slice(None)}
        return own.at[lax.rem(c, SLOTS), sel["x"], sel["z"], sel["y"], k]

    def split(half):
        return pl.ds(16 * half, 16 - 8 * half)

    def part(phase, k, c, a, half):
        s = lax.rem(c, SLOTS)
        if phase == 0:
            return own_at(c, k, a, half)
        if phase == 1:
            return buf2.at[s, k, a, pl.ds(2 * half, 2)]
        return buf3.at[s, k, a, split(half)]

    def land(phase, k, c, m):
        s = lax.rem(c, SLOTS)
        if phase == 0:
            return ra[k].at[s, m]
        return rb.at[s, k, m] if phase == 1 else rc.at[s, k, m, pl.ds(0, 8 if m in (1, 2, 5) else 16)]

    def copies(phase, k, c, step):
        axis = ORDERS[k][phase]
        p = pos[axis]
        right, left, far = lax.rem(p + 1, 4), lax.rem(p + 3, 4), lax.rem(p + 2, 4)
        to_r, to_l = {"fsdp": shifted(me, pos, axis, 1)}, {"fsdp": shifted(me, pos, axis, 3)}
        if step == 0:
            table = ((0, part(phase, k, c, far, 0), to_r), (1, part(phase, k, c, far, 1), to_l),
                     (2, part(phase, k, c, right, 1), to_r), (3, part(phase, k, c, left, 0), to_l))
        else:
            table = ((4, land(phase, k, c, 0), to_r), (5, land(phase, k, c, 1), to_l))
        return [(m, remote(src, land(phase, k, c, m), ssem.at[phase, lax.rem(c, SLOTS), k, m], rsem.at[phase, lax.rem(c, SLOTS), k, m], dev)) for m, src, dev in table]

    def first(phase, c):
        for k in range(COLORS):
            for _, cp in copies(phase, k, c, 0):
                cp.start()

    def second(phase, c):
        for k in range(COLORS):
            axis = ORDERS[k][phase]
            p = pos[axis]
            right, left = lax.rem(p + 1, 4), lax.rem(p + 3, 4)
            one = copies(phase, k, c, 0)
            for m, a in ((0, right), (1, left)):
                one[m][1].wait_recv()
                dst = land(phase, k, c, m)
                dst[...] = dst[...] + part(phase, k, c, a, m)[...]
            for _, cp in copies(phase, k, c, 1):
                cp.start()

    def last(phase, c, store):
        for k in range(COLORS):
            p = pos[ORDERS[k][phase]]
            one, two = copies(phase, k, c, 0), copies(phase, k, c, 1)
            for m, cp in one[2:] + two:
                cp.wait_recv()
            for half, (m, n) in enumerate(((4, 3), (5, 2))):
                store(k, half, part(phase, k, c, p, half)[...] + land(phase, k, c, m)[...] + land(phase, k, c, n)[...])
            for m, cp in one + two:
                cp.wait_send()

    def store1(s):
        def put(k, half, v):
            if k == 2:
                for i in range(2):
                    buf2[s, k, 2 * half + i] = v[i]
            else:
                for i in range(2):
                    buf2[s, k, 2 * half + i] = v[:, i]
        return put

    def store2(s):
        def put(k, half, v):
            buf3[s, k, pl.ds(2 * half, 2)] = v
        return put

    def store3(c):
        s = lax.rem(c, SLOTS)

        def put(k, half, v):
            low = rows * k + 16 * half
            size = 16 - 8 * half
            for x in range(NX):
                lo, hi = max(low, x * cols), min(low + size, x * cols + cols)
                if lo < hi:
                    piece[s, x, lo - x * cols:hi - x * cols] = v[lo - low:hi - low]
        return put

    def home(c, x):
        return grad_ref.at[:, pl.ds(pl.multiple_of(x * quarter + c * lanes, LANE), lanes)]

    def hand_out(c):
        p = pos["x"]
        return [remote(piece.at[lax.rem(c, SLOTS), lax.rem(p + d, NX)], home(c, p), psend.at[c, d - 1], precv.at[c, d - 1],
                       {"fsdp": shifted(me, pos, "x", d)}) for d in (1, 2, 3)]

    def finish_piece(c):
        last(2, c, store3(c))
        home(c, pos["x"])[...] = piece[lax.rem(c, SLOTS), pos["x"]]
        for cp in hand_out(c):
            cp.start()

    def collect(c):
        for cp in hand_out(c):
            cp.wait()

    half_rows = tokens // 2
    mine = pl.ds(pl.multiple_of(tp * half_rows, half_rows), half_rows)
    other = pl.ds(pl.multiple_of((1 - tp) * half_rows, half_rows), half_rows)

    def swap_dxn():
        return remote(dxn.at[other], dxn_in, xsend.at[0], xrecv.at[0], partner)

    def swap_dh():
        return remote(dh_ref.at[mine], dh_ref.at[mine], xsend.at[1], xrecv.at[1], partner)

    def swap_look(back):
        if back:
            return remote(look_ref.at[mine], look_ref.at[mine], xsend.at[3], xrecv.at[3], partner)
        return remote(look_ref.at[other], look_in, xsend.at[2], xrecv.at[2], partner)

    def finish_look():
        swap_look(False).wait()
        pl.semaphore_signal(look_free, device_id=partner, device_id_type=MESH)
        look_ref[mine] = look_ref[mine] + look_in[...]

    def finish_hidden():
        swap_dxn().wait()
        sums[...] = jnp.zeros_like(sums)
        gain = gain_ref[...]

        def block(b, acc):
            lo = span(b * LANE, LANE)
            r = span(tp * half_rows + b * LANE, LANE)
            inv = stat_ref[r, 1:2]
            hn = h_ref[r].astype(F32) * inv
            dx = dxn[r] + dxn_in[lo]
            g_dir = dx * gain
            mean = jnp.mean(g_dir * hn, axis=1, keepdims=True)
            dh_ref[r] = (inv * (g_dir - hn * mean)).astype(BF16)
            return acc + jnp.sum(dx * hn, axis=0, keepdims=True)

        dg = lax.fori_loop(0, half_rows // LANE, block, jnp.zeros((1, width), F32))
        n = width // LANE
        for i in range(n):
            sums[pl.ds(i, 1), :] = dg[:, LANE * i:LANE * i + LANE]
        sums[pl.ds(n, 1), :] = loss_ref[...]
        swap_dh().start()

    def sum_copies(phase):
        if phase == 3:
            peers = [partner]
        else:
            peers = [{"fsdp": shifted(me, pos, "xyz"[phase], d)} for d in (1, 2, 3)]
        return [remote(sums, sums_in.at[phase, j], sum_send.at[phase, j], sum_recv.at[phase, j], n) for j, n in enumerate(peers)]

    def sum_start(phase):
        for cp in sum_copies(phase):
            cp.start()

    def sum_end(phase):
        cps = sum_copies(phase)
        for cp in cps:
            cp.wait()
        if phase == 3:
            small_ref[...] = sums[...] + sums_in[3, 0]
        else:
            sums[...] = sums[...] + sums_in[phase, 0] + sums_in[phase, 1] + sums_in[phase, 2]

    dxn[...] = jnp.zeros_like(dxn)
    look_ref[...] = jnp.zeros_like(look_ref)
    for cp in loads(0):
        cp.start()
    ticks = chunks + 7

    def tick(t, carry):
        @pl.when(t < chunks)
        def _():
            produce(t, lax.rem(t, SLOTS))

        @pl.when(t == 0)
        def _():
            pl.semaphore_wait(barrier, len(everyone))

        @pl.when(t >= 1)
        def _():
            for i in range(6):
                pl.semaphore_wait(credit.at[i])

        def stage(delay, run):
            c = t - delay
            @pl.when(jnp.logical_and(c >= 0, c < chunks))
            def _():
                run(c)

        def s2(c):
            last(0, c, store1(lax.rem(c, SLOTS)))
            first(1, c)

        def s4(c):
            last(1, c, store2(lax.rem(c, SLOTS)))
            first(2, c)

        stage(0, lambda c: first(0, c))
        @pl.when(t == chunks - 1)
        def _():
            swap_dxn().start()
            swap_look(False).start()
        stage(7, collect)
        stage(6, finish_piece)
        stage(5, lambda c: second(2, c))
        stage(4, s4)
        stage(3, lambda c: second(1, c))
        stage(2, s2)
        stage(1, lambda c: second(0, c))

        @pl.when(t == chunks)
        def _():
            finish_hidden()
        @pl.when(t == chunks + 1)
        def _():
            sum_start(0)
            swap_dh().wait()
            finish_look()
        for phase in range(3):
            @pl.when(t == chunks + 2 + phase)
            def _():
                if phase == 0:
                    pl.semaphore_wait(look_free)
                    swap_look(True).start()
                if phase == 2:
                    swap_look(True).wait()
                sum_end(phase)
                sum_start(phase + 1)
        @pl.when(t == chunks + 5)
        def _():
            sum_end(3)

        @pl.when(t < ticks - 1)
        def _():
            for i, n in enumerate(near):
                pl.semaphore_signal(credit.at[i], device_id=n, device_id_type=MESH)
        return carry

    lax.fori_loop(0, ticks, tick, 0)


def gradients(total_tokens, emb_scale, u, table, xt, ids, stat, h, gain, loss):
    tokens, vocab = u.shape
    width = h.shape[1]
    quarter = vocab // NX
    lanes = quarter // CHUNKS
    rows = width // 48
    vm = pl.BlockSpec(memory_space=pltpu.VMEM)
    hbm = pl.BlockSpec(memory_space=pl.ANY)
    dma = pltpu.SemaphoreType.DMA
    return pl.pallas_call(
        functools.partial(grad_kernel, total_tokens, emb_scale),
        out_shape=[jax.ShapeDtypeStruct((width // (NX * NX * NX), vocab), F32), jax.ShapeDtypeStruct((tokens, width), BF16), jax.ShapeDtypeStruct((16, LANE), F32), jax.ShapeDtypeStruct((tokens, width), BF16)],
        in_specs=[hbm, hbm] + [vm] * 6,
        out_specs=[vm, vm, vm, vm],
        scratch_shapes=[
            pltpu.VMEM((SLOTS, 4, 4, 4, COLORS, rows, lanes), F32),
            pltpu.VMEM((SLOTS, COLORS, 4, 4, rows, lanes), F32),
            pltpu.VMEM((SLOTS, COLORS, 4, rows, lanes), F32),
            pltpu.VMEM((SLOTS, 6, 4, 2, rows, lanes), F32),
            pltpu.VMEM((SLOTS, 6, 4, 2, rows, lanes), F32),
            pltpu.VMEM((SLOTS, 6, 2, 4, rows, lanes), F32),
            pltpu.VMEM((SLOTS, COLORS, 6, 2, rows, lanes), F32),
            pltpu.VMEM((SLOTS, COLORS, 6, 16, lanes), F32),
            pltpu.VMEM((2, tokens, lanes), F32),
            pltpu.VMEM((2, width, lanes), BF16),
            pltpu.VMEM((2 * tokens, lanes), BF16),
            pltpu.VMEM((tokens, width), F32),
            pltpu.VMEM((tokens // 2, width), F32),
            pltpu.VMEM((tokens // 2, width), BF16),
            pltpu.VMEM((SLOTS, NX, width // (NX * NX * NX), lanes), F32),
            pltpu.VMEM((16, LANE), F32),
            pltpu.VMEM((4, 3, 16, LANE), F32),
            dma((2, 2)),
            dma((3, SLOTS, COLORS, 6)),
            dma((3, SLOTS, COLORS, 6)),
            dma((4,)),
            dma((4,)),
            dma((4, 3)),
            dma((4, 3)),
            dma((CHUNKS, 3)),
            dma((CHUNKS, 3)),
            pltpu.SemaphoreType.REGULAR((6,)),
            pltpu.SemaphoreType.REGULAR,
        ],
        compiler_params=pltpu.CompilerParams(collective_id=2, has_side_effects=True, vmem_limit_bytes=63 * 2**20),
    )(u, table, xt, ids, stat, h, gain, loss)


def table_kernel(emb_ref, norm_ref, ids_ref, h_hbm, g_hbm, u_ref, table_ref, xt_hbm, stat_ref, gain_ref, loss_ref,
                 xin, mid, tab, norms, norms_in, xn, rhs, ubuf, acc, sums, sums_in, xt_ref, h_ref, g_ref,
                 big_sem, ex_send, ex_recv, nsend, nrecv, ssem, rsem, psend, precv, usem, tsem):
    me = lax.axis_index("fsdp")
    tp = lax.axis_index("tp")
    pos = coords(me)
    tokens, width = h_ref.shape
    parts, block, lanes = tab.shape[0], tab.shape[5], tab.shape[6]
    sub = emb_ref.shape[2]
    cols = emb_ref.shape[1]
    quarter = NX * sub
    peers = {a: [{"fsdp": shifted(me, pos, a, d)} for d in (1, 2, 3)] for a in "xyz"}
    partner = {"tp": 1 - tp}
    plane = NX * NX
    here = lax.rem(me, plane)
    field = [{"fsdp": me - here + lax.rem(here + d, plane)} for d in range(1, plane)]
    big = (pltpu.make_async_copy(h_hbm, h_ref, big_sem.at[0]), pltpu.make_async_copy(g_hbm, g_ref, big_sem.at[1]),
           pltpu.make_async_copy(xt_ref, xt_hbm, big_sem.at[2]))
    big[0].start()
    big[1].start()
    greet(field + peers["z"] + [partner])

    def exchange():
        return [remote(emb_ref.at[lax.rem(here + d + 1, plane)], xin.at[here], ex_send.at[d], ex_recv.at[d], n) for d, n in enumerate(field)]

    def norm_copies(j):
        return [remote(norms, norms_in.at[j, d], nsend.at[j, d], nrecv.at[j, d], peers["xyz"[j]][d]) for d in range(3)]

    def norm_start(j):
        for cp in norm_copies(j):
            cp.start()

    def norm_end(j):
        for cp in norm_copies(j):
            cp.wait()
        norms[...] = norms[...] + norms_in[j, 0] + norms_in[j, 1] + norms_in[j, 2]

    norms[...] = norm_ref[...]
    for cp in exchange():
        cp.start()
    norm_start(0)
    xin[here] = emb_ref[here]
    for cp in exchange():
        cp.wait()
    for i in range(plane):
        mid[pl.ds(cols * i, cols), :] = xin[i].astype(F32)
    for c in range(parts):
        for k in range(COLORS):
            tab[c, pos["x"], pos["y"], pos["z"], k] = mid[block * k:block * k + block, lanes * c:lanes * c + lanes].astype(BF16)

    def region(e, kind, k, a, half):
        o = ORDERS[k]
        if kind == 0:
            sel = {o[0]: pos[o[0]], o[1]: pos[o[1]], o[2]: a}
            return tab.at[:, sel["x"], sel["y"], sel["z"], k, pl.ds(half * (block // 2), block // 2)]
        if kind == 1:
            sel = {o[0]: pos[o[0]], o[1]: a, o[2]: pl.ds(2 * half, 2)}
            return tab.at[e - 1, sel["x"], sel["y"], sel["z"], k]
        sel = {o[0]: a, o[1]: pl.ds(2 * half, 2), o[2]: slice(None)}
        return tab.at[e - 1 - parts, sel["x"], sel["y"], sel["z"], k]

    def copies(e, k, step):
        kind = 2 if not isinstance(e, int) or e > parts else min(e, 1)
        axis = ORDERS[k][2 - kind]
        p = pos[axis]
        right, left = lax.rem(p + 1, 4), lax.rem(p + 3, 4)
        to_r, to_l = {"fsdp": shifted(me, pos, axis, 1)}, {"fsdp": shifted(me, pos, axis, 3)}
        if step == 0:
            plan = ((0, p, 0, to_r), (1, p, 1, to_l), (2, p, 1, to_r), (3, p, 0, to_l))
        else:
            plan = ((4, left, 0, to_r), (5, right, 1, to_l))
        return [remote(region(e, kind, k, a, half), region(e, kind, k, a, half), ssem.at[e, k, m], rsem.at[e, k, m], dev)
                for m, a, half, dev in plan]

    def begin(e):
        for k in range(COLORS):
            for cp in copies(e, k, 0):
                cp.start()

    def forward(e):
        for k in range(COLORS):
            one, two = copies(e, k, 0), copies(e, k, 1)
            one[0].wait_recv()
            two[0].start()
            one[1].wait_recv()
            two[1].start()

    def arrive(e):
        for k in range(COLORS):
            one, two = copies(e, k, 0), copies(e, k, 1)
            for cp in one[2:] + two:
                cp.wait_recv()
            for cp in one + two:
                cp.wait_send()

    bulk = 1 + parts
    norm_end(0)
    norm_start(1)
    begin(0)
    norm_end(1)
    norm_start(2)
    forward(0)
    arrive(0)
    for c in range(parts):
        begin(1 + c)
    norm_end(2)
    n = width // LANE
    gain = 1.0 + jnp.concatenate([norms[pl.ds(i, 1), :] for i in range(n)], axis=1)
    gain_ref[...] = gain

    def normalize(b, carry):
        r = span(b * LANE, LANE)
        hw = h_ref[r].astype(F32)
        inv = lax.rsqrt(jnp.mean(hw * hw, axis=1, keepdims=True) + NORM_EPS)
        v = (hw * inv * gain_ref[...]).astype(BF16)
        xn[r] = v
        stat_ref[r, 1:2] = inv
        xt_ref[:, r] = v.T
        xt_ref[:, span(tokens + b * LANE, LANE)] = g_ref[r].T
        return carry

    big[0].wait()
    big[1].wait()
    lax.fori_loop(0, tokens // LANE, normalize, 0)
    acc[...] = jnp.zeros_like(acc)
    for c in range(parts):
        forward(1 + c)
        if c >= 1:
            arrive(c)
            if c <= 2:
                begin(bulk + c - 1)
    arrive(parts)
    forward(bulk)

    def u_out(i):
        c, p = lax.div(i, 8), lax.rem(i, 8)
        s = lax.rem(i, 2)
        base = lax.div(p, 2) * quarter + lax.rem(p, 2) * (2 * sub) + c * lanes
        return [pltpu.make_async_copy(ubuf.at[s, j], u_ref.at[:, pl.ds(pl.multiple_of(base + j * sub, LANE), lanes)], usem.at[s, j]) for j in range(2)]

    def table_out(c):
        cps = []
        for x in range(4):
            for y in range(4):
                at = pl.ds(pl.multiple_of(x * quarter + y * sub + c * lanes, LANE), lanes)
                cps.append(pltpu.make_async_copy(tab.at[c, x, y], table_ref.at[:, :, :, at], tsem.at[x, y]))
        return cps

    def chunk(c, carry):
        arrive(c + bulk)

        @pl.when(c + 2 < parts)
        def _():
            begin(c + 2 + bulk)

        @pl.when(c >= 1)
        def _():
            for cp in table_out(c - 1):
                cp.wait()
        for cp in table_out(c):
            cp.start()

        def pair(p, carry):
            i = c * 8 + p
            s = lax.rem(i, 2)
            x, y = lax.div(p, 2), lax.rem(p, 2) * 2
            for j in range(2):
                rhs[:, lanes * j:lanes * j + lanes] = tab[c, x, y + j].reshape(width, lanes)

            @pl.when(i >= 2)
            def _():
                for cp in u_out(i - 2):
                    cp.wait()
            base = x * quarter + y * sub + c * lanes
            lane = lax.broadcasted_iota(jnp.int32, (ROWS, 2 * lanes), 1)
            ids = lane + base + jnp.where(lane >= lanes, sub - lanes, 0)

            def rows(b, carry):
                r = span(b * ROWS, ROWS)
                z = jnp.dot(xn[r], rhs[...], preferred_element_type=F32)
                u = jnp.tanh(z * (1.0 / SOFT_CAP))
                for j in range(2):
                    ubuf[s, j, r] = u[:, lanes * j:lanes * j + lanes]
                capped = SOFT_CAP * u
                e = jnp.exp(capped - SOFT_CAP)
                hit = jnp.where(ids_ref[r, 1:2] == ids, capped, 0.0)
                acc[0, r] = acc[0, r] + e[:, :lanes] + e[:, lanes:]
                acc[1, r] = acc[1, r] + hit[:, :lanes] + hit[:, lanes:]
                return carry

            lax.fori_loop(0, tokens // ROWS, rows, 0, unroll=True)
            for cp in u_out(i):
                cp.start()

            @pl.when(jnp.logical_and(p == NX - 1, c + 1 < parts))
            def _():
                forward(c + 1 + bulk)
            return carry

        lax.fori_loop(0, 8, pair, 0)
        return carry

    big[2].start()
    lax.fori_loop(0, parts, chunk, 0)
    lane = lax.broadcasted_iota(jnp.int32, (tokens, LANE), 1)
    sums[...] = jnp.where(lane == 0, jnp.sum(acc[0], axis=1, keepdims=True), jnp.sum(acc[1], axis=1, keepdims=True))
    big[2].wait()
    swap = remote(sums, sums_in, psend, precv, partner)
    swap.start()
    for cp in u_out(parts * 8 - 2) + u_out(parts * 8 - 1) + table_out(parts - 1):
        cp.wait()
    swap.wait()
    both = sums[...] + sums_in[...]
    lse = jnp.log(both[:, 0:1]) + SOFT_CAP
    stat_ref[:, 0:1] = lse
    loss_ref[...] = jnp.broadcast_to(0.5 * jnp.sum(lse - both[:, 1:2], axis=0, keepdims=True), (1, LANE))


def table_pass(emb, norm, h, g, ids):
    tokens, width = h.shape
    sub = emb.shape[2]
    cols = emb.shape[1]
    quarter = NX * sub
    vocab = NX * quarter
    block = width // 12
    parts = sub // LANE
    vm = pl.BlockSpec(memory_space=pltpu.VMEM)
    hbm = pl.BlockSpec(memory_space=pl.ANY)
    dma = pltpu.SemaphoreType.DMA
    u, table, xt, stat, gain, loss = pl.pallas_call(
        table_kernel,
        out_shape=[
            jax.ShapeDtypeStruct((tokens, vocab), F32),
            jax.ShapeDtypeStruct((4, COLORS, block, vocab), BF16),
            jax.ShapeDtypeStruct((width, 2 * tokens), BF16),
            jax.ShapeDtypeStruct((tokens, 2), F32),
            jax.ShapeDtypeStruct((1, width), F32),
            jax.ShapeDtypeStruct((1, LANE), F32),
        ],
        in_specs=[vm] * 3 + [hbm] * 2,
        out_specs=[hbm, hbm, hbm, vm, vm, vm],
        scratch_shapes=[
            pltpu.VMEM((NX * NX, cols, sub), BF16),
            pltpu.VMEM((NX * NX * cols, sub), F32),
            pltpu.VMEM((parts, 4, 4, 4, COLORS, block, LANE), BF16),
            pltpu.VMEM((16, LANE), F32),
            pltpu.VMEM((3, 3, 16, LANE), F32),
            pltpu.VMEM((tokens, width), BF16),
            pltpu.VMEM((width, ROWS), BF16),
            pltpu.VMEM((2, 2, tokens, LANE), F32),
            pltpu.VMEM((2, tokens, LANE), F32),
            pltpu.VMEM((tokens, LANE), F32),
            pltpu.VMEM((tokens, LANE), F32),
            pltpu.VMEM((width, 2 * tokens), BF16),
            pltpu.VMEM((tokens, width), BF16),
            pltpu.VMEM((tokens, width), BF16),
            dma((3,)),
            dma((NX * NX,)),
            dma((NX * NX,)),
            dma((3, 3)),
            dma((3, 3)),
            dma((1 + 2 * parts, COLORS, 6)),
            dma((1 + 2 * parts, COLORS, 6)),
            dma,
            dma,
            dma((2, 2)),
            dma((4, 4)),
        ],
        compiler_params=pltpu.CompilerParams(collective_id=1, has_side_effects=True, vmem_limit_bytes=63 * 2**20),
    )(emb, norm, ids, h, g)
    return u, table.reshape(width, vocab), xt, stat, gain, loss


def math_scale(width):
    import numpy as np
    return float(np.asarray(math.sqrt(width), BF16).astype(np.float32))


def solution(mesh):
    fsdp_size = mesh.shape["fsdp"]

    def device_step(emb_shard, tok_ids, lab_ids, h_last, g_embed, norm_w):
        vocab_rows, cols = emb_shard.shape
        batch_loc, seq_len, width = h_last.shape
        tok_count = batch_loc * seq_len
        total_tokens = tok_count * fsdp_size
        quarter = vocab_rows // NX
        row_start = lax.axis_index("tp") * vocab_rows
        me = lax.axis_index("fsdp")

        emb = emb_shard.T.astype(BF16).reshape(cols, NX, NX, quarter // NX).transpose(2, 1, 0, 3).reshape(NX * NX, cols, quarter // NX)
        norm = lax.dynamic_update_slice(jnp.zeros((16 * LANE,), F32), norm_w, (me * cols,)).reshape(16, LANE)
        ids = jnp.stack([tok_ids.reshape(tok_count) - row_start, lab_ids.reshape(tok_count) - row_start], axis=1)
        h = h_last.reshape(tok_count, width)
        g = g_embed.reshape(tok_count, width)
        u, table, xt, stat, gain, loss = table_pass(emb, norm, h, g, ids)
        grad, d_hidden, small, x_emb = gradients(total_tokens, math_scale(width), u, table, xt, ids, stat, h, gain, loss)
        loss_val = small[width // LANE, 0] / total_tokens
        d_norm_w = lax.dynamic_slice(small.reshape(-1), (me * cols,), (cols,))
        d_table = grad.T
        return (x_emb.reshape(batch_loc, seq_len, width), loss_val, d_hidden.reshape(batch_loc, seq_len, width), d_norm_w, d_table)

    spec_tok = P("fsdp", None)
    spec_act = P("fsdp", None, None)
    return jax.shard_map(device_step, mesh=mesh, in_specs=(P("tp", "fsdp"), spec_tok, spec_tok, spec_act, spec_act, P("fsdp")), out_specs=(spec_act, P(), spec_act, P("fsdp"), P("tp", "fsdp")), check_vma=False)
```

```python
import functools
import math
import jax
import jax.numpy as jnp
from jax import lax
from jax.experimental import pallas as pl
from jax.experimental.pallas import tpu as pltpu
from jax.sharding import PartitionSpec as P

SOFT_CAP = 30.0
NORM_EPS = 1e-6
MESH = pl.DeviceIdType.MESH
NX = 4
COLORS = 3
SLOTS = 3
CHUNKS = 8
ORDERS = (("x", "y", "z"), ("y", "z", "x"), ("z", "x", "y"))
STEP = {"x": 1, "y": 4, "z": 16}
LANE = 128
ROWS = 256
F32, BF16 = jnp.float32, jnp.bfloat16


def coords(me):
    return {"x": lax.rem(me, 4), "y": lax.rem(lax.div(me, 4), 4), "z": lax.div(me, 16)}


def shifted(me, pos, axis, d):
    there = lax.rem(pos[axis] + d, 4)
    return me + (there - pos[axis]) * STEP[axis]


def span(start, size):
    return pl.ds(pl.multiple_of(start, size), size)


def remote(src, dst, send, recv, device):
    return pltpu.make_async_remote_copy(src_ref=src, dst_ref=dst, send_sem=send, recv_sem=recv, device_id=device, device_id_type=MESH)


def greet(devices):
    barrier = pltpu.get_barrier_semaphore()
    for n in devices:
        pl.semaphore_signal(barrier, device_id=n, device_id_type=MESH)
    pl.semaphore_wait(barrier, len(devices))


def grad_kernel(total_tokens, emb_scale, u_ref, table_ref, xt_ref, ids_ref, stat_ref, h_ref, gain_ref, loss_ref,
                grad_ref, dh_ref, small_ref, look_ref, own, buf2, buf3, ra0, ra1, ra2, rb, rc, ubuf, tbuf, dz, dxn, dxn_in, look_in, piece, sums, sums_in,
                load_sem, ssem, rsem, xsend, xrecv, sum_send, sum_recv, psend, precv, credit, look_free):
    me = lax.axis_index("fsdp")
    tp = lax.axis_index("tp")
    pos = coords(me)
    chunks = CHUNKS
    lanes = own.shape[-1]
    rows = own.shape[-2]
    tokens, width = h_ref.shape
    vocab = u_ref.shape[1]
    cols = grad_ref.shape[0]
    quarter = vocab // NX
    ra = (ra0, ra1, ra2)
    near = [{"fsdp": shifted(me, pos, a, d)} for a in "xyz" for d in (1, 3)]
    partner = {"tp": 1 - tp}
    everyone = near + [{"fsdp": shifted(me, pos, a, 2)} for a in "xyz"] + [partner]
    barrier = pltpu.get_barrier_semaphore()
    for n in everyone:
        pl.semaphore_signal(barrier, device_id=n, device_id_type=MESH)

    def loads(i):
        c, q = lax.div(i, NX), lax.rem(i, NX)
        s = lax.rem(i, 2)
        at = pl.ds(pl.multiple_of(q * quarter + c * lanes, LANE), lanes)
        return (pltpu.make_async_copy(u_ref.at[:, at], ubuf.at[s], load_sem.at[s, 0]),
                pltpu.make_async_copy(table_ref.at[:, at], tbuf.at[s], load_sem.at[s, 1]))

    def produce(c, slot):
        def one(q, carry):
            i = c * NX + q
            s = lax.rem(i, 2)
            for cp in loads(i):
                cp.wait()

            @pl.when(i + 1 < chunks * NX)
            def _():
                for cp in loads(i + 1):
                    cp.start()

            first_id = q * quarter + c * lanes

            def block(b, carry):
                r = span(b * ROWS, ROWS)
                ids = lax.broadcasted_iota(jnp.int32, (ROWS, lanes), 1) + first_id
                u = ubuf[s, r]
                prob = jnp.exp(SOFT_CAP * u - stat_ref[r, 0:1])
                hit = (ids_ref[r, 1:2] == ids).astype(F32)
                d = ((prob - hit) * (1.0 - u * u) * (1.0 / total_tokens)).astype(BF16)
                dz[r] = d
                pick = jnp.where(ids_ref[r, 0:1] == ids, emb_scale, 0.0).astype(BF16)
                dz[pl.ds(pl.multiple_of(tokens + b * ROWS, ROWS), ROWS)] = pick
                part = lax.dot_general(d, tbuf[s], (((1,), (1,)), ((), ())), preferred_element_type=F32)
                dxn[r] = dxn[r] + part
                found = lax.dot_general(pick, tbuf[s], (((1,), (1,)), ((), ())), preferred_element_type=F32)
                look_ref[r] = look_ref[r] + found.astype(BF16)
                return carry

            lax.fori_loop(0, tokens // ROWS, block, 0, unroll=True)

            def out(z, carry):
                w = width // 2
                v = jnp.dot(xt_ref[pl.ds(pl.multiple_of(z * w, 32), w), :], dz[...], preferred_element_type=F32)
                own[slot, q, pl.ds(2 * z, 2)] = v.reshape(2, 4, COLORS, rows, lanes)
                return carry

            lax.fori_loop(0, 2, out, 0, unroll=True)
            return carry

        lax.fori_loop(0, NX, one, 0)

    def own_at(c, k, a1, half):
        o = ORDERS[k]
        sel = {o[0]: a1, o[1]: pl.ds(2 * half, 2), o[2]: slice(None)}
        return own.at[lax.rem(c, SLOTS), sel["x"], sel["z"], sel["y"], k]

    def split(half):
        return pl.ds(16 * half, 16 - 8 * half)

    def part(phase, k, c, a, half):
        s = lax.rem(c, SLOTS)
        if phase == 0:
            return own_at(c, k, a, half)
        if phase == 1:
            return buf2.at[s, k, a, pl.ds(2 * half, 2)]
        return buf3.at[s, k, a, split(half)]

    def land(phase, k, c, m):
        s = lax.rem(c, SLOTS)
        if phase == 0:
            return ra[k].at[s, m]
        return rb.at[s, k, m] if phase == 1 else rc.at[s, k, m, pl.ds(0, 8 if m in (1, 2, 5) else 16)]

    def copies(phase, k, c, step):
        axis = ORDERS[k][phase]
        p = pos[axis]
        right, left, far = lax.rem(p + 1, 4), lax.rem(p + 3, 4), lax.rem(p + 2, 4)
        to_r, to_l = {"fsdp": shifted(me, pos, axis, 1)}, {"fsdp": shifted(me, pos, axis, 3)}
        if step == 0:
            table = ((0, part(phase, k, c, far, 0), to_r), (1, part(phase, k, c, far, 1), to_l),
                     (2, part(phase, k, c, right, 1), to_r), (3, part(phase, k, c, left, 0), to_l))
        else:
            table = ((4, land(phase, k, c, 0), to_r), (5, land(phase, k, c, 1), to_l))
        return [(m, remote(src, land(phase, k, c, m), ssem.at[phase, lax.rem(c, SLOTS), k, m], rsem.at[phase, lax.rem(c, SLOTS), k, m], dev)) for m, src, dev in table]

    def first(phase, c):
        for k in range(COLORS):
            for _, cp in copies(phase, k, c, 0):
                cp.start()

    def second(phase, c):
        for k in range(COLORS):
            axis = ORDERS[k][phase]
            p = pos[axis]
            right, left = lax.rem(p + 1, 4), lax.rem(p + 3, 4)
            one = copies(phase, k, c, 0)
            for m, a in ((0, right), (1, left)):
                one[m][1].wait_recv()
                dst = land(phase, k, c, m)
                dst[...] = dst[...] + part(phase, k, c, a, m)[...]
            for _, cp in copies(phase, k, c, 1):
                cp.start()

    def last(phase, c, store):
        for k in range(COLORS):
            p = pos[ORDERS[k][phase]]
            one, two = copies(phase, k, c, 0), copies(phase, k, c, 1)
            for m, cp in one[2:] + two:
                cp.wait_recv()
            for half, (m, n) in enumerate(((4, 3), (5, 2))):
                store(k, half, part(phase, k, c, p, half)[...] + land(phase, k, c, m)[...] + land(phase, k, c, n)[...])
            for m, cp in one + two:
                cp.wait_send()

    def store1(s):
        def put(k, half, v):
            if k == 2:
                for i in range(2):
                    buf2[s, k, 2 * half + i] = v[i]
            else:
                for i in range(2):
                    buf2[s, k, 2 * half + i] = v[:, i]
        return put

    def store2(s):
        def put(k, half, v):
            buf3[s, k, pl.ds(2 * half, 2)] = v
        return put

    def store3(c):
        s = lax.rem(c, SLOTS)

        def put(k, half, v):
            low = rows * k + 16 * half
            size = 16 - 8 * half
            for x in range(NX):
                lo, hi = max(low, x * cols), min(low + size, x * cols + cols)
                if lo < hi:
                    piece[s, x, lo - x * cols:hi - x * cols] = v[lo - low:hi - low]
        return put

    def home(c, x):
        return grad_ref.at[:, pl.ds(pl.multiple_of(x * quarter + c * lanes, LANE), lanes)]

    def hand_out(c):
        p = pos["x"]
        return [remote(piece.at[lax.rem(c, SLOTS), lax.rem(p + d, NX)], home(c, p), psend.at[c, d - 1], precv.at[c, d - 1],
                       {"fsdp": shifted(me, pos, "x", d)}) for d in (1, 2, 3)]

    def finish_piece(c):
        last(2, c, store3(c))
        home(c, pos["x"])[...] = piece[lax.rem(c, SLOTS), pos["x"]]
        for cp in hand_out(c):
            cp.start()

    def collect(c):
        for cp in hand_out(c):
            cp.wait()

    half_rows = tokens // 2
    mine = pl.ds(pl.multiple_of(tp * half_rows, half_rows), half_rows)
    other = pl.ds(pl.multiple_of((1 - tp) * half_rows, half_rows), half_rows)

    def swap_dxn():
        return remote(dxn.at[other], dxn_in, xsend.at[0], xrecv.at[0], partner)

    def swap_dh():
        return remote(dh_ref.at[mine], dh_ref.at[mine], xsend.at[1], xrecv.at[1], partner)

    def swap_look(back):
        if back:
            return remote(look_ref.at[mine], look_ref.at[mine], xsend.at[3], xrecv.at[3], partner)
        return remote(look_ref.at[other], look_in, xsend.at[2], xrecv.at[2], partner)

    def finish_look():
        swap_look(False).wait()
        pl.semaphore_signal(look_free, device_id=partner, device_id_type=MESH)
        look_ref[mine] = look_ref[mine] + look_in[...]

    def finish_hidden():
        swap_dxn().wait()
        sums[...] = jnp.zeros_like(sums)
        gain = gain_ref[...]

        def block(b, acc):
            lo = span(b * LANE, LANE)
            r = span(tp * half_rows + b * LANE, LANE)
            inv = stat_ref[r, 1:2]
            hn = h_ref[r].astype(F32) * inv
            dx = dxn[r] + dxn_in[lo]
            g_dir = dx * gain
            mean = jnp.mean(g_dir * hn, axis=1, keepdims=True)
            dh_ref[r] = (inv * (g_dir - hn * mean)).astype(BF16)
            return acc + jnp.sum(dx * hn, axis=0, keepdims=True)

        dg = lax.fori_loop(0, half_rows // LANE, block, jnp.zeros((1, width), F32))
        n = width // LANE
        for i in range(n):
            sums[pl.ds(i, 1), :] = dg[:, LANE * i:LANE * i + LANE]
        sums[pl.ds(n, 1), :] = loss_ref[...]
        swap_dh().start()

    def sum_copies(phase):
        if phase == 3:
            peers = [partner]
        else:
            peers = [{"fsdp": shifted(me, pos, "xyz"[phase], d)} for d in (1, 2, 3)]
        return [remote(sums, sums_in.at[phase, j], sum_send.at[phase, j], sum_recv.at[phase, j], n) for j, n in enumerate(peers)]

    def sum_start(phase):
        for cp in sum_copies(phase):
            cp.start()

    def sum_end(phase):
        cps = sum_copies(phase)
        for cp in cps:
            cp.wait()
        if phase == 3:
            small_ref[...] = sums[...] + sums_in[3, 0]
        else:
            sums[...] = sums[...] + sums_in[phase, 0] + sums_in[phase, 1] + sums_in[phase, 2]

    for cp in loads(0):
        cp.start()
    dxn[...] = jnp.zeros_like(dxn)
    look_ref[...] = jnp.zeros_like(look_ref)
    ticks = chunks + 7

    def tick(t, carry):
        @pl.when(t < chunks)
        def _():
            produce(t, lax.rem(t, SLOTS))

        @pl.when(t == 0)
        def _():
            pl.semaphore_wait(barrier, len(everyone))

        @pl.when(t >= 1)
        def _():
            for i in range(6):
                pl.semaphore_wait(credit.at[i])

        def stage(delay, run):
            c = t - delay
            @pl.when(jnp.logical_and(c >= 0, c < chunks))
            def _():
                run(c)

        def s2(c):
            last(0, c, store1(lax.rem(c, SLOTS)))
            first(1, c)

        def s4(c):
            last(1, c, store2(lax.rem(c, SLOTS)))
            first(2, c)

        stage(1, lambda c: second(0, c))
        stage(0, lambda c: first(0, c))
        @pl.when(t == chunks - 1)
        def _():
            swap_dxn().start()
            swap_look(False).start()
        stage(7, collect)
        stage(6, finish_piece)
        stage(5, lambda c: second(2, c))
        stage(4, s4)
        stage(3, lambda c: second(1, c))
        stage(2, s2)

        @pl.when(t == chunks)
        def _():
            finish_hidden()
        @pl.when(t == chunks + 1)
        def _():
            sum_start(0)
            swap_dh().wait()
            finish_look()
        for phase in range(3):
            @pl.when(t == chunks + 2 + phase)
            def _():
                if phase == 0:
                    pl.semaphore_wait(look_free)
                    swap_look(True).start()
                if phase == 2:
                    swap_look(True).wait()
                sum_end(phase)
                sum_start(phase + 1)
        @pl.when(t == chunks + 5)
        def _():
            sum_end(3)

        @pl.when(t < ticks - 1)
        def _():
            for i, n in enumerate(near):
                pl.semaphore_signal(credit.at[i], device_id=n, device_id_type=MESH)
        return carry

    lax.fori_loop(0, ticks, tick, 0)


def gradients(total_tokens, emb_scale, u, table, xt, ids, stat, h, gain, loss):
    tokens, vocab = u.shape
    width = h.shape[1]
    quarter = vocab // NX
    lanes = quarter // CHUNKS
    rows = width // 48
    vm = pl.BlockSpec(memory_space=pltpu.VMEM)
    hbm = pl.BlockSpec(memory_space=pl.ANY)
    dma = pltpu.SemaphoreType.DMA
    return pl.pallas_call(
        functools.partial(grad_kernel, total_tokens, emb_scale),
        out_shape=[jax.ShapeDtypeStruct((width // (NX * NX * NX), vocab), F32), jax.ShapeDtypeStruct((tokens, width), BF16), jax.ShapeDtypeStruct((16, LANE), F32), jax.ShapeDtypeStruct((tokens, width), BF16)],
        in_specs=[hbm, hbm] + [vm] * 6,
        out_specs=[vm, vm, vm, vm],
        scratch_shapes=[
            pltpu.VMEM((SLOTS, 4, 4, 4, COLORS, rows, lanes), F32),
            pltpu.VMEM((SLOTS, COLORS, 4, 4, rows, lanes), F32),
            pltpu.VMEM((SLOTS, COLORS, 4, rows, lanes), F32),
            pltpu.VMEM((SLOTS, 6, 4, 2, rows, lanes), F32),
            pltpu.VMEM((SLOTS, 6, 4, 2, rows, lanes), F32),
            pltpu.VMEM((SLOTS, 6, 2, 4, rows, lanes), F32),
            pltpu.VMEM((SLOTS, COLORS, 6, 2, rows, lanes), F32),
            pltpu.VMEM((SLOTS, COLORS, 6, 16, lanes), F32),
            pltpu.VMEM((2, tokens, lanes), F32),
            pltpu.VMEM((2, width, lanes), BF16),
            pltpu.VMEM((2 * tokens, lanes), BF16),
            pltpu.VMEM((tokens, width), F32),
            pltpu.VMEM((tokens // 2, width), F32),
            pltpu.VMEM((tokens // 2, width), BF16),
            pltpu.VMEM((SLOTS, NX, width // (NX * NX * NX), lanes), F32),
            pltpu.VMEM((16, LANE), F32),
            pltpu.VMEM((4, 3, 16, LANE), F32),
            dma((2, 2)),
            dma((3, SLOTS, COLORS, 6)),
            dma((3, SLOTS, COLORS, 6)),
            dma((4,)),
            dma((4,)),
            dma((4, 3)),
            dma((4, 3)),
            dma((CHUNKS, 3)),
            dma((CHUNKS, 3)),
            pltpu.SemaphoreType.REGULAR((6,)),
            pltpu.SemaphoreType.REGULAR,
        ],
        compiler_params=pltpu.CompilerParams(collective_id=2, has_side_effects=True, vmem_limit_bytes=63 * 2**20),
    )(u, table, xt, ids, stat, h, gain, loss)


def table_kernel(emb_ref, norm_ref, ids_ref, h_hbm, g_hbm, u_ref, table_ref, xt_hbm, stat_ref, gain_ref, loss_ref,
                 xin, mid, tab, norms, norms_in, xn, rhs, ubuf, acc, sums, sums_in, xt_ref, h_ref, g_ref,
                 big_sem, ex_send, ex_recv, nsend, nrecv, ssem, rsem, psend, precv, usem, tsem):
    me = lax.axis_index("fsdp")
    tp = lax.axis_index("tp")
    pos = coords(me)
    tokens, width = h_ref.shape
    parts, block, lanes = tab.shape[0], tab.shape[5], tab.shape[6]
    sub = emb_ref.shape[2]
    cols = emb_ref.shape[1]
    quarter = NX * sub
    peers = {a: [{"fsdp": shifted(me, pos, a, d)} for d in (1, 2, 3)] for a in "xyz"}
    partner = {"tp": 1 - tp}
    plane = NX * NX
    here = lax.rem(me, plane)
    field = [{"fsdp": me - here + lax.rem(here + d, plane)} for d in range(1, plane)]
    big = (pltpu.make_async_copy(h_hbm, h_ref, big_sem.at[0]), pltpu.make_async_copy(g_hbm, g_ref, big_sem.at[1]),
           pltpu.make_async_copy(xt_ref, xt_hbm, big_sem.at[2]))
    big[0].start()
    big[1].start()
    greet(field + peers["z"] + [partner])

    def exchange():
        return [remote(emb_ref.at[lax.rem(here + d + 1, plane)], xin.at[here], ex_send.at[d], ex_recv.at[d], n) for d, n in enumerate(field)]

    def norm_copies(j):
        return [remote(norms, norms_in.at[j, d], nsend.at[j, d], nrecv.at[j, d], peers["xyz"[j]][d]) for d in range(3)]

    def norm_start(j):
        for cp in norm_copies(j):
            cp.start()

    def norm_end(j):
        for cp in norm_copies(j):
            cp.wait()
        norms[...] = norms[...] + norms_in[j, 0] + norms_in[j, 1] + norms_in[j, 2]

    norms[...] = norm_ref[...]
    for cp in exchange():
        cp.start()
    norm_start(0)
    xin[here] = emb_ref[here]
    for cp in exchange():
        cp.wait()
    for i in range(plane):
        mid[pl.ds(cols * i, cols), :] = xin[i].astype(F32)
    for c in range(parts):
        for k in range(COLORS):
            tab[c, pos["x"], pos["y"], pos["z"], k] = mid[block * k:block * k + block, lanes * c:lanes * c + lanes].astype(BF16)

    def region(e, kind, k, a, half):
        o = ORDERS[k]
        if kind == 0:
            sel = {o[0]: pos[o[0]], o[1]: pos[o[1]], o[2]: a}
            return tab.at[:, sel["x"], sel["y"], sel["z"], k, pl.ds(half * (block // 2), block // 2)]
        if kind == 1:
            sel = {o[0]: pos[o[0]], o[1]: a, o[2]: pl.ds(2 * half, 2)}
            return tab.at[e - 1, sel["x"], sel["y"], sel["z"], k]
        sel = {o[0]: a, o[1]: pl.ds(2 * half, 2), o[2]: slice(None)}
        return tab.at[e - 1 - parts, sel["x"], sel["y"], sel["z"], k]

    def copies(e, k, step):
        kind = 2 if not isinstance(e, int) or e > parts else min(e, 1)
        axis = ORDERS[k][2 - kind]
        p = pos[axis]
        right, left = lax.rem(p + 1, 4), lax.rem(p + 3, 4)
        to_r, to_l = {"fsdp": shifted(me, pos, axis, 1)}, {"fsdp": shifted(me, pos, axis, 3)}
        if step == 0:
            plan = ((0, p, 0, to_r), (1, p, 1, to_l), (2, p, 1, to_r), (3, p, 0, to_l))
        else:
            plan = ((4, left, 0, to_r), (5, right, 1, to_l))
        return [remote(region(e, kind, k, a, half), region(e, kind, k, a, half), ssem.at[e, k, m], rsem.at[e, k, m], dev)
                for m, a, half, dev in plan]

    def begin(e):
        for k in range(COLORS):
            for cp in copies(e, k, 0):
                cp.start()

    def forward(e):
        for k in range(COLORS):
            one, two = copies(e, k, 0), copies(e, k, 1)
            one[0].wait_recv()
            two[0].start()
            one[1].wait_recv()
            two[1].start()

    def arrive(e):
        for k in range(COLORS):
            one, two = copies(e, k, 0), copies(e, k, 1)
            for cp in one[2:] + two:
                cp.wait_recv()
            for cp in one + two:
                cp.wait_send()

    bulk = 1 + parts
    norm_end(0)
    norm_start(1)
    begin(0)
    norm_end(1)
    norm_start(2)
    forward(0)
    arrive(0)
    for c in range(parts):
        begin(1 + c)
    norm_end(2)
    n = width // LANE
    gain = 1.0 + jnp.concatenate([norms[pl.ds(i, 1), :] for i in range(n)], axis=1)
    gain_ref[...] = gain

    def normalize(b, carry):
        r = span(b * LANE, LANE)
        hw = h_ref[r].astype(F32)
        inv = lax.rsqrt(jnp.mean(hw * hw, axis=1, keepdims=True) + NORM_EPS)
        v = (hw * inv * gain_ref[...]).astype(BF16)
        xn[r] = v
        stat_ref[r, 1:2] = inv
        xt_ref[:, r] = v.T
        xt_ref[:, span(tokens + b * LANE, LANE)] = g_ref[r].T
        return carry

    big[0].wait()
    big[1].wait()
    lax.fori_loop(0, tokens // LANE, normalize, 0)
    acc[...] = jnp.zeros_like(acc)
    for c in range(parts):
        forward(1 + c)
        if c >= 1:
            arrive(c)
            if c <= 2:
                begin(bulk + c - 1)
    arrive(parts)
    forward(bulk)

    def u_out(i):
        c, p = lax.div(i, 8), lax.rem(i, 8)
        s = lax.rem(i, 2)
        base = lax.div(p, 2) * quarter + lax.rem(p, 2) * (2 * sub) + c * lanes
        return [pltpu.make_async_copy(ubuf.at[s, j], u_ref.at[:, pl.ds(pl.multiple_of(base + j * sub, LANE), lanes)], usem.at[s, j]) for j in range(2)]

    def table_out(c):
        cps = []
        for x in range(4):
            for y in range(4):
                at = pl.ds(pl.multiple_of(x * quarter + y * sub + c * lanes, LANE), lanes)
                cps.append(pltpu.make_async_copy(tab.at[c, x, y], table_ref.at[:, :, :, at], tsem.at[x, y]))
        return cps

    def chunk(c, carry):
        arrive(c + bulk)

        @pl.when(c + 2 < parts)
        def _():
            begin(c + 2 + bulk)

        @pl.when(c >= 1)
        def _():
            for cp in table_out(c - 1):
                cp.wait()
        for cp in table_out(c):
            cp.start()

        def pair(p, carry):
            i = c * 8 + p
            s = lax.rem(i, 2)
            x, y = lax.div(p, 2), lax.rem(p, 2) * 2
            for j in range(2):
                rhs[:, lanes * j:lanes * j + lanes] = tab[c, x, y + j].reshape(width, lanes)

            @pl.when(i >= 2)
            def _():
                for cp in u_out(i - 2):
                    cp.wait()
            base = x * quarter + y * sub + c * lanes
            lane = lax.broadcasted_iota(jnp.int32, (ROWS, 2 * lanes), 1)
            ids = lane + base + jnp.where(lane >= lanes, sub - lanes, 0)

            def rows(b, carry):
                r = span(b * ROWS, ROWS)
                z = jnp.dot(xn[r], rhs[...], preferred_element_type=F32)
                u = jnp.tanh(z * (1.0 / SOFT_CAP))
                for j in range(2):
                    ubuf[s, j, r] = u[:, lanes * j:lanes * j + lanes]
                capped = SOFT_CAP * u
                e = jnp.exp(capped - SOFT_CAP)
                hit = jnp.where(ids_ref[r, 1:2] == ids, capped, 0.0)
                acc[0, r] = acc[0, r] + e[:, :lanes] + e[:, lanes:]
                acc[1, r] = acc[1, r] + hit[:, :lanes] + hit[:, lanes:]
                return carry

            lax.fori_loop(0, tokens // ROWS, rows, 0, unroll=True)
            for cp in u_out(i):
                cp.start()

            @pl.when(jnp.logical_and(p == NX - 1, c + 1 < parts))
            def _():
                forward(c + 1 + bulk)
            return carry

        lax.fori_loop(0, 8, pair, 0)
        return carry

    big[2].start()
    lax.fori_loop(0, parts, chunk, 0)
    lane = lax.broadcasted_iota(jnp.int32, (tokens, LANE), 1)
    sums[...] = jnp.where(lane == 0, jnp.sum(acc[0], axis=1, keepdims=True), jnp.sum(acc[1], axis=1, keepdims=True))
    big[2].wait()
    swap = remote(sums, sums_in, psend, precv, partner)
    swap.start()
    for cp in u_out(parts * 8 - 2) + u_out(parts * 8 - 1) + table_out(parts - 1):
        cp.wait()
    swap.wait()
    both = sums[...] + sums_in[...]
    lse = jnp.log(both[:, 0:1]) + SOFT_CAP
    stat_ref[:, 0:1] = lse
    loss_ref[...] = jnp.broadcast_to(0.5 * jnp.sum(lse - both[:, 1:2], axis=0, keepdims=True), (1, LANE))


def table_pass(emb, norm, h, g, ids):
    tokens, width = h.shape
    sub = emb.shape[2]
    cols = emb.shape[1]
    quarter = NX * sub
    vocab = NX * quarter
    block = width // 12
    parts = sub // LANE
    vm = pl.BlockSpec(memory_space=pltpu.VMEM)
    hbm = pl.BlockSpec(memory_space=pl.ANY)
    dma = pltpu.SemaphoreType.DMA
    u, table, xt, stat, gain, loss = pl.pallas_call(
        table_kernel,
        out_shape=[
            jax.ShapeDtypeStruct((tokens, vocab), F32),
            jax.ShapeDtypeStruct((4, COLORS, block, vocab), BF16),
            jax.ShapeDtypeStruct((width, 2 * tokens), BF16),
            jax.ShapeDtypeStruct((tokens, 2), F32),
            jax.ShapeDtypeStruct((1, width), F32),
            jax.ShapeDtypeStruct((1, LANE), F32),
        ],
        in_specs=[vm] * 3 + [hbm] * 2,
        out_specs=[hbm, hbm, hbm, vm, vm, vm],
        scratch_shapes=[
            pltpu.VMEM((NX * NX, cols, sub), BF16),
            pltpu.VMEM((NX * NX * cols, sub), F32),
            pltpu.VMEM((parts, 4, 4, 4, COLORS, block, LANE), BF16),
            pltpu.VMEM((16, LANE), F32),
            pltpu.VMEM((3, 3, 16, LANE), F32),
            pltpu.VMEM((tokens, width), BF16),
            pltpu.VMEM((width, ROWS), BF16),
            pltpu.VMEM((2, 2, tokens, LANE), F32),
            pltpu.VMEM((2, tokens, LANE), F32),
            pltpu.VMEM((tokens, LANE), F32),
            pltpu.VMEM((tokens, LANE), F32),
            pltpu.VMEM((width, 2 * tokens), BF16),
            pltpu.VMEM((tokens, width), BF16),
            pltpu.VMEM((tokens, width), BF16),
            dma((3,)),
            dma((NX * NX,)),
            dma((NX * NX,)),
            dma((3, 3)),
            dma((3, 3)),
            dma((1 + 2 * parts, COLORS, 6)),
            dma((1 + 2 * parts, COLORS, 6)),
            dma,
            dma,
            dma((2, 2)),
            dma((4, 4)),
        ],
        compiler_params=pltpu.CompilerParams(collective_id=1, has_side_effects=True, vmem_limit_bytes=63 * 2**20),
    )(emb, norm, ids, h, g)
    return u, table.reshape(width, vocab), xt, stat, gain, loss


def math_scale(width):
    import numpy as np
    return float(np.asarray(math.sqrt(width), BF16).astype(np.float32))


def solution(mesh):
    fsdp_size = mesh.shape["fsdp"]

    def device_step(emb_shard, tok_ids, lab_ids, h_last, g_embed, norm_w):
        vocab_rows, cols = emb_shard.shape
        batch_loc, seq_len, width = h_last.shape
        tok_count = batch_loc * seq_len
        total_tokens = tok_count * fsdp_size
        quarter = vocab_rows // NX
        row_start = lax.axis_index("tp") * vocab_rows
        me = lax.axis_index("fsdp")

        emb = emb_shard.T.astype(BF16).reshape(cols, NX, NX, quarter // NX).transpose(2, 1, 0, 3).reshape(NX * NX, cols, quarter // NX)
        norm = lax.dynamic_update_slice(jnp.zeros((16 * LANE,), F32), norm_w, (me * cols,)).reshape(16, LANE)
        ids = jnp.stack([tok_ids.reshape(tok_count) - row_start, lab_ids.reshape(tok_count) - row_start], axis=1)
        h = h_last.reshape(tok_count, width)
        g = g_embed.reshape(tok_count, width)
        u, table, xt, stat, gain, loss = table_pass(emb, norm, h, g, ids)
        grad, d_hidden, small, x_emb = gradients(total_tokens, math_scale(width), u, table, xt, ids, stat, h, gain, loss)
        loss_val = small[width // LANE, 0] / total_tokens
        d_norm_w = lax.dynamic_slice(small.reshape(-1), (me * cols,), (cols,))
        d_table = grad.T
        return (x_emb.reshape(batch_loc, seq_len, width), loss_val, d_hidden.reshape(batch_loc, seq_len, width), d_norm_w, d_table)

    spec_tok = P("fsdp", None)
    spec_act = P("fsdp", None, None)
    return jax.shard_map(device_step, mesh=mesh, in_specs=(P("tp", "fsdp"), spec_tok, spec_tok, spec_act, spec_act, P("fsdp")), out_specs=(spec_act, P(), spec_act, P("fsdp"), P("tp", "fsdp")), check_vma=False)
```
